16 devices in a mesh: rep: 4 (over y, z, core), dp: 4 (over x).
Axes of the slice: x: 4, y: 2, z: 1, core: 2. Of those that a mesh axis runs over, the one named last changes fastest.
The devices are a block of a 4x4x8 slice.
Arguments:
- g_w_gate: bfloat16 [16, 2, 896, 2560], P(('rep', 'dp')), parts along dimension 0
- g_w_up: bfloat16 [16, 2, 896, 2560], P(('rep', 'dp')), parts along dimension 0
- g_w_down: bfloat16 [16, 2, 2560, 896], P(('rep', 'dp')), parts along dimension 0
- w_gate: bfloat16 [2, 896, 2560], replicated
- w_up: bfloat16 [2, 896, 2560], replicated
- w_down: bfloat16 [2, 2560, 896], replicated
- m_w_gate: float32 [2, 896, 2560], P(None, 'dp')
- m_w_up: float32 [2, 896, 2560], P(None, 'dp')
- m_w_down: float32 [2, 2560, 896], P(None, 'dp')
- v_w_gate: float32 [2, 896, 2560], P(None, 'dp')
- v_w_up: float32 [2, 896, 2560], P(None, 'dp')
- v_w_down: float32 [2, 2560, 896], P(None, 'dp')
Outputs:
- output 1: bfloat16 [8, 896, 2560], P('rep'), parts along dimension 0
- output 2: bfloat16 [8, 896, 2560], P('rep'), parts along dimension 0
- output 3: bfloat16 [8, 2560, 896], P('rep'), parts along dimension 0
- output 4: float32 [8, 896, 2560], P('rep', 'dp'), parts along dimension 0
- output 5: float32 [8, 896, 2560], P('rep', 'dp'), parts along dimension 0
- output 6: float32 [8, 2560, 896], P('rep', 'dp'), parts along dimension 0
- output 7: float32 [8, 896, 2560], P('rep', 'dp'), parts along dimension 0
- output 8: float32 [8, 896, 2560], P('rep', 'dp'), parts along dimension 0
- output 9: float32 [8, 2560, 896], P('rep', 'dp'), parts along dimension 0
There are 4 independent parts. The reference program is written for one: setup_inputs(seed, part) draws one part's arguments, and reference() takes and returns one part's arrays. A program takes and returns all parts, laid end to end along the dimension named above; an argument that names none is the same for every part.
All inputs are finite; a program needn't handle non-finite values.
Results may differ from the reference program's by a relative error of at most 0.022.
Values are sent between devices in bfloat16 or wider.
A program may use at most 768 MiB of HBM per device.

```python
import jax
import jax.numpy as jnp
from jax import lax

DEVICES = 4
D = 896
FF = 2560
LAYERS = 2
NAMES = ("w_gate", "w_up", "w_down")
SHAPES = {"w_gate": (LAYERS, D, FF), "w_up": (LAYERS, D, FF), "w_down": (LAYERS, FF, D)}


def setup_inputs(seed: int = 0, part: int = 0) -> dict:
    kz, *keys = jax.random.split(jax.random.key(seed), 1 + 5 * len(NAMES))
    loud = 2.0 ** jax.random.uniform(kz, (), jnp.float32, -1.0, 1.0)
    drawn = {}
    for name, key, both in zip(NAMES, keys[:3], keys[3:6], strict=True):
        own = jax.random.normal(jax.random.fold_in(key, part), (DEVICES, *SHAPES[name]), jnp.float32)
        shared = jax.random.normal(jax.random.fold_in(both, part), SHAPES[name], jnp.float32)
        drawn["g_" + name] = (loud * (0.7 * shared / DEVICES + 0.7 * own * DEVICES**-0.5)).astype(jnp.bfloat16)
    for name, key in zip(NAMES, keys[6:9], strict=True):
        drawn[name] = (jax.random.normal(key, SHAPES[name], jnp.float32) * SHAPES[name][1] ** -0.5).astype(jnp.bfloat16)
    for name, key in zip(NAMES, keys[9:12], strict=True):
        drawn["m_" + name] = loud * 0.5 * jax.random.normal(key, SHAPES[name], jnp.float32)
    for name, key in zip(NAMES, keys[12:15], strict=True):
        drawn["v_" + name] = loud * loud * jax.random.uniform(key, SHAPES[name], jnp.float32, 0.5, 1.5)
    return drawn


def adamw(w, m, v, g):
    m = 0.9 * m + 0.1 * g
    v = 0.95 * v + 0.05 * g * g
    step = m * lax.rsqrt(v + 1e-8) + 0.1 * w
    return (w - 0.02 * step).astype(jnp.bfloat16), m, v


def reference(g_w_gate, g_w_up, g_w_down, w_gate, w_up, w_down, m_w_gate, m_w_up, m_w_down, v_w_gate, v_w_up, v_w_down):
    def total(terms):
        return lax.scan(lambda so_far, term: (so_far + term.astype(jnp.float32), None), jnp.zeros(terms.shape[1:], jnp.float32), terms)[0]

    gradients = [total(terms).astype(jnp.bfloat16).astype(jnp.float32) for terms in (g_w_gate, g_w_up, g_w_down)]
    new = [
        adamw(w.astype(jnp.float32), m, v, g)
        for w, m, v, g in zip((w_gate, w_up, w_down), (m_w_gate, m_w_up, m_w_down), (v_w_gate, v_w_up, v_w_down), gradients, strict=True)
    ]
    return tuple(one[which] for which in range(3) for one in new)
```

```python
import functools

import jax
import jax.numpy as jnp
from jax import lax
from jax.experimental import pallas as pl
from jax.experimental.pallas import tpu as pltpu
from jax.sharding import PartitionSpec as P

MESH = pl.DeviceIdType.MESH
BF16, F32 = jnp.bfloat16, jnp.float32
SENT = ("far_s", "far_r", "rel_s", "rel_r", "dir_s", "dir_r", "fwd_s", "fwd_r")
LOCAL = ("term", "own", "w", "m", "v", "g_out", "w_out")
BOTH_WAYS = ("near_s", "near_r")
SEMAPHORES = (*SENT, *LOCAL, *BOTH_WAYS)


def moments(m, v, g):
    return 0.9 * m + 0.1 * g, 0.95 * v + 0.05 * g * g


def weight(w, m, v):
    return w - 0.02 * (m * lax.rsqrt(v + 1e-8) + 0.1 * w)


def columns(width):
    parts = -(-width // 1024)
    while width % (parts * 128):
        parts += 1
    return [slice(i * (width // parts), (i + 1) * (width // parts)) for i in range(parts)]


def tiled(shape, body):
    def row(i, carry):
        rows = pl.ds(pl.multiple_of(i * 16, 16), 16)
        for cols in columns(shape[1]):
            body(rows, cols)
        return carry

    lax.fori_loop(0, shape[0] // 16, row, 0)


def kernel(n, layers, gathered, *refs):
    count = len(gathered)
    refs = list(refs)
    take = lambda k: [refs.pop(0) for _ in range(k)]
    g, w, m, v = take(count), take(count), take(count), take(count)
    g_out, w_out = take(count), take(count)
    far, rel, direct, term, own, new = (take(count) for _ in range(6))
    m_buf, v_buf = take(count), take(count)
    sem = dict(zip(SEMAPHORES, refs, strict=True))

    me = lax.axis_index("dp")
    right, left = lax.rem(me + 1, n), lax.rem(me + n - 1, n)
    opposite = lax.rem(me + 2, n)
    ahead, behind = (right, left), (left, right)

    barrier = pltpu.get_barrier_semaphore()
    for peer in (left, right):
        pl.semaphore_signal(barrier, inc=1, device_id={"dp": peer}, device_id_type=MESH)
    pl.semaphore_wait(barrier, 2)

    chunks = [(k, layer) for k in range(count) for layer in range(layers)]
    pending = []

    def rows(k, block, side):
        half = far[k].shape[2]
        return pl.ds(pl.multiple_of((2 * block + side) * half, 16), half)

    def send(src, dst, send_sem, recv_sem, peer):
        copy = pltpu.make_async_remote_copy(src, dst, send_sem, recv_sem, device_id={"dp": peer}, device_id_type=MESH)
        copy.start()
        pending.append(copy.wait_send)
        return copy

    def local(src, dst, s):
        copy = pltpu.make_async_copy(src, dst, s)
        copy.start()
        return copy

    sent, loads, steps = {}, {}, {}

    def first(c):
        k, l = chunks[c]
        for side in (0, 1):
            sent["far", c, side] = send(
                g[k].at[0, l, rows(k, opposite, side)], far[k].at[l, side], sem["far_s"].at[c, side], sem["far_r"].at[c, side], ahead[side]
            )
        for side in (0, 1):
            sent["dir", c, side] = send(
                g[k].at[0, l, rows(k, behind[side], side)], direct[k].at[l, side], sem["dir_s"].at[c, side], sem["dir_r"].at[c, side], behind[side]
            )
        for side in (0, 1):
            loads["term", c, side] = local(g[k].at[0, l, rows(k, ahead[side], side)], term[k].at[l, side], sem["term"].at[c, side])
        for side in (0, 1):
            loads["own", c, side] = local(g[k].at[0, l, rows(k, me, side)], own[k].at[l, side], sem["own"].at[c, side])
            loads["w", c, side] = local(w[k].at[l, rows(k, me, side)], new[k].at[l, side], sem["w"].at[c, side])

    def load_moments(c, side):
        k, l = chunks[c]
        half = far[k].shape[2]
        here = pl.ds(side * half, half)
        steps[c, side] = (
            local(m[k].at[l, here], m_buf[k].at[side], sem["m"].at[c, side]),
            local(v[k].at[l, here], v_buf[k].at[side], sem["v"].at[c, side]),
        )

    def relay(c):
        k, l = chunks[c]
        for side in (0, 1):
            sent["far", c, side].wait_recv()
            loads["term", c, side].wait()
            sums, mine = far[k].at[l, side], term[k].at[l, side]

            def add(r, cols):
                sums[r, cols] = (sums[r, cols].astype(F32) + mine[r, cols].astype(F32)).astype(BF16)

            tiled(sums.shape, add)
            sent["rel", c, side] = send(sums, rel[k].at[l, side], sem["rel_s"].at[c, side], sem["rel_r"].at[c, side], ahead[side])

    def step(c):
        k, l = chunks[c]
        half = far[k].shape[2]
        for side in (0, 1):
            sent["dir", c, side].wait_recv()
            sent["rel", c, side].wait_recv()
            loads["own", c, side].wait()
            loads["w", c, side].wait()
            for load in steps[c, side]:
                load.wait()
            a, b, o, x = (array[k].at[l, side] for array in (rel, direct, own, new))
            ms, vs = m_buf[k].at[side], v_buf[k].at[side]

            def update(r, cols):
                total = (a[r, cols].astype(F32) + b[r, cols].astype(F32) + o[r, cols].astype(F32)).astype(BF16)
                o[r, cols] = total
                m_new, v_new = moments(ms[r, cols], vs[r, cols], total.astype(F32))
                x[r, cols] = weight(x[r, cols].astype(F32), m_new, v_new).astype(BF16)

            tiled(o.shape, update)
            here = pl.ds(side * half, half)
            pending.append(local(o, g_out[k].at[l, here], sem["g_out"].at[c, side]).wait)
            if gathered[k]:
                place = w_out[k].at[l, rows(k, me, side)]
                for way, peer in enumerate((ahead[side], behind[side])):
                    sent["near", c, side, way] = send(x, place, sem["near_s"].at[c, side, way], sem["near_r"].at[c, side, way], peer)
            else:
                place = w_out[k].at[l, here]
            pending.append(local(x, place, sem["w_out"].at[c, side]).wait)
            if c + 1 < len(chunks):
                load_moments(c + 1, side)

    def forward(c):
        k, l = chunks[c]
        if not gathered[k]:
            return
        for side in (0, 1):
            sent["near", c, side, 0].wait_recv()
            place = w_out[k].at[l, rows(k, behind[side], side)]
            sent["fwd", c, side] = send(place, place, sem["fwd_s"].at[c, side], sem["fwd_r"].at[c, side], ahead[side])

    last = len(chunks)
    for c in range(min(2, last)):
        first(c)
    for side in (0, 1):
        load_moments(0, side)
    for c in range(last + 2):
        if c + 2 < last:
            first(c + 2)
        if c < last:
            relay(c)
        if 0 <= c - 1 < last:
            step(c - 1)
        if 0 <= c - 2 < last:
            forward(c - 2)
    for key, copy in sent.items():
        if key[0] == "fwd" or (key[0] == "near" and key[3] == 1):
            copy.wait_recv()
    for wait in pending:
        wait()


def reduce_and_step(n, gathered, terms, weights, m, v):
    layers = m[0].shape[0]
    count = len(terms)
    chunks = count * layers
    pieces = [(layers, 2, one.shape[1] // 2, one.shape[2]) for one in m]
    blocks = [jax.ShapeDtypeStruct(one.shape, BF16) for one in m]
    out_shape = blocks + [
        jax.ShapeDtypeStruct(w.shape if whole else one.shape, BF16) for w, one, whole in zip(weights, blocks, gathered, strict=True)
    ]
    sems = [pltpu.SemaphoreType.DMA((chunks, 2, 2) if name in BOTH_WAYS else (chunks, 2)) for name in SEMAPHORES]
    return pl.pallas_call(
        functools.partial(kernel, n, layers, gathered),
        out_shape=out_shape,
        in_specs=[pl.BlockSpec(memory_space=pl.ANY)] * (4 * count),
        out_specs=[pl.BlockSpec(memory_space=pl.ANY)] * (2 * count),
        scratch_shapes=[pltpu.VMEM(p, BF16) for _ in range(6) for p in pieces]
        + [pltpu.VMEM(p[1:], F32) for _ in range(2) for p in pieces]
        + sems,
        compiler_params=pltpu.CompilerParams(collective_id=0, has_side_effects=True, vmem_limit_bytes=66_000_000),
        name="reduce_and_step",
    )(*terms, *weights, *m, *v)


GATHERED = (True, True, True)


def solution(mesh):
    n = mesh.shape["dp"]

    def body(*arrays):
        terms, weights, m, v = (arrays[i : i + 3] for i in (0, 3, 6, 9))
        out = reduce_and_step(n, GATHERED, terms, weights, m, v)
        sums, new = out[:3], out[3:]
        pairs = [moments(m, v, g.astype(F32)) for m, v, g in zip(m, v, sums, strict=True)]
        return (*new, *(one[0] for one in pairs), *(one[1] for one in pairs))

    all_of, cut = P(None, None, None), P(None, "dp", None)
    return jax.shard_map(
        body,
        mesh=mesh,
        in_specs=(P(("rep", "dp"), None, None, None),) * 3 + (all_of,) * 3 + (cut,) * 6,
        out_specs=(P("rep", None, None),) * 3 + (P("rep", "dp", None),) * 6,
        check_vma=False,
    )
```

```python
import functools

import jax
import jax.numpy as jnp
from jax import lax
from jax.experimental import pallas as pl
from jax.experimental.pallas import tpu as pltpu
from jax.sharding import PartitionSpec as P


MESH = pl.DeviceIdType.MESH
BF16, F32 = jnp.bfloat16, jnp.float32
SENT = ("far_s", "far_r", "rel_s", "rel_r", "dir_s", "dir_r", "fwd_s", "fwd_r")
LOCAL = ("term", "own", "w", "m", "v", "g_out", "w_out")
BOTH_WAYS = ("near_s", "near_r")
SEMAPHORES = (*SENT, *LOCAL, *BOTH_WAYS)


def moments(m, v, g):
    return 0.9 * m + 0.1 * g, 0.95 * v + 0.05 * g * g


def weight(w, m, v):
    return w - 0.02 * (m * lax.rsqrt(v + 1e-8) + 0.1 * w)


def columns(width):
    parts = -(-width // 1024)
    while width % (parts * 128):
        parts += 1
    return [slice(i * (width // parts), (i + 1) * (width // parts)) for i in range(parts)]


def tiled(shape, body):
    def row(i, carry):
        rows = pl.ds(pl.multiple_of(i * 16, 16), 16)
        for cols in columns(shape[1]):
            body(rows, cols)
        return carry

    lax.fori_loop(0, shape[0] // 16, row, 0)


def kernel(n, layers, gathered, *refs):
    count = len(gathered)
    refs = list(refs)
    take = lambda k: [refs.pop(0) for _ in range(k)]
    g, w, m, v = take(count), take(count), take(count), take(count)
    g_out = take(count)
    w_out = [take(1)[0] if whole else [[refs.pop(0) for _ in range(2)] for _ in range(layers)] for whole in gathered]
    far, rel, direct, term, own, new = (take(count) for _ in range(6))
    m_buf, v_buf = take(count), take(count)
    sem = dict(zip(SEMAPHORES, refs, strict=True))

    me = lax.axis_index("dp")
    right, left = lax.rem(me + 1, n), lax.rem(me + n - 1, n)
    opposite = lax.rem(me + 2, n)
    ahead, behind = (right, left), (left, right)

    barrier = pltpu.get_barrier_semaphore()
    for peer in (left, right):
        pl.semaphore_signal(barrier, inc=1, device_id={"dp": peer}, device_id_type=MESH)
    pl.semaphore_wait(barrier, 2)

    chunks = [(k, layer) for k in range(count) for layer in range(layers)]
    pending = []

    def rows(k, block, side):
        half = far[k].shape[2]
        return pl.ds(pl.multiple_of((2 * block + side) * half, 16), half)

    def send(src, dst, send_sem, recv_sem, peer):
        copy = pltpu.make_async_remote_copy(src, dst, send_sem, recv_sem, device_id={"dp": peer}, device_id_type=MESH)
        copy.start()
        pending.append(copy.wait_send)
        return copy

    def local(src, dst, s):
        copy = pltpu.make_async_copy(src, dst, s)
        copy.start()
        return copy

    sent, loads, steps = {}, {}, {}

    def first(c):
        k, l = chunks[c]
        for side in (0, 1):
            sent["far", c, side] = send(
                g[k].at[0, l, rows(k, opposite, side)], far[k].at[l, side], sem["far_s"].at[c, side], sem["far_r"].at[c, side], ahead[side]
            )
        for side in (0, 1):
            sent["dir", c, side] = send(
                g[k].at[0, l, rows(k, behind[side], side)], direct[k].at[l, side], sem["dir_s"].at[c, side], sem["dir_r"].at[c, side], behind[side]
            )
        for side in (0, 1):
            loads["term", c, side] = local(g[k].at[0, l, rows(k, ahead[side], side)], term[k].at[l, side], sem["term"].at[c, side])
        for side in (0, 1):
            loads["own", c, side] = local(g[k].at[0, l, rows(k, me, side)], own[k].at[l, side], sem["own"].at[c, side])
            loads["w", c, side] = local(w[k].at[l, rows(k, me, side)], new[k].at[l, side], sem["w"].at[c, side])

    def load_moments(c, side):
        k, l = chunks[c]
        half = far[k].shape[2]
        here = pl.ds(side * half, half)
        steps[c, side] = (
            local(m[k].at[l, here], m_buf[k].at[side], sem["m"].at[c, side]),
            local(v[k].at[l, here], v_buf[k].at[side], sem["v"].at[c, side]),
        )

    def relay(c):
        k, l = chunks[c]
        for side in (0, 1):
            sent["far", c, side].wait_recv()
            loads["term", c, side].wait()
            sums, mine = far[k].at[l, side], term[k].at[l, side]

            def add(r, cols):
                sums[r, cols] = (sums[r, cols].astype(F32) + mine[r, cols].astype(F32)).astype(BF16)

            tiled(sums.shape, add)
            sent["rel", c, side] = send(sums, rel[k].at[l, side], sem["rel_s"].at[c, side], sem["rel_r"].at[c, side], ahead[side])

    def step(c):
        k, l = chunks[c]
        half = far[k].shape[2]
        for side in (0, 1):
            sent["dir", c, side].wait_recv()
            sent["rel", c, side].wait_recv()
            loads["own", c, side].wait()
            loads["w", c, side].wait()
            for load in steps[c, side]:
                load.wait()
            a, b, o, x = (array[k].at[l, side] for array in (rel, direct, own, new))
            ms, vs = m_buf[k].at[side], v_buf[k].at[side]

            def update(r, cols):
                total = (a[r, cols].astype(F32) + b[r, cols].astype(F32) + o[r, cols].astype(F32)).astype(BF16)
                o[r, cols] = total
                m_new, v_new = moments(ms[r, cols], vs[r, cols], total.astype(F32))
                x[r, cols] = weight(x[r, cols].astype(F32), m_new, v_new).astype(BF16)

            tiled(o.shape, update)
            here = pl.ds(side * half, half)
            pending.append(local(o, g_out[k].at[l, here], sem["g_out"].at[c, side]).wait)
            if gathered[k]:
                place = w_out[k].at[l, rows(k, me, side)]
                for way, peer in enumerate((ahead[side], behind[side])):
                    sent["near", c, side, way] = send(x, place, sem["near_s"].at[c, side, way], sem["near_r"].at[c, side, way], peer)
            else:
                place = w_out[k][l][side]
            pending.append(local(x, place, sem["w_out"].at[c, side]).wait)
            if c + 1 < len(chunks):
                load_moments(c + 1, side)

    def forward(c):
        k, l = chunks[c]
        if not gathered[k]:
            return
        for side in (0, 1):
            sent["near", c, side, 0].wait_recv()
            place = w_out[k].at[l, rows(k, behind[side], side)]
            sent["fwd", c, side] = send(place, place, sem["fwd_s"].at[c, side], sem["fwd_r"].at[c, side], ahead[side])

    last = len(chunks)
    for c in range(min(2, last)):
        first(c)
    for side in (0, 1):
        load_moments(0, side)
    for c in range(last + 2):
        if c + 2 < last:
            first(c + 2)
        if c < last:
            relay(c)
        if 0 <= c - 1 < last:
            step(c - 1)
        if 0 <= c - 2 < last:
            forward(c - 2)
    for key, copy in sent.items():
        if key[0] == "fwd" or (key[0] == "near" and key[3] == 1):
            copy.wait_recv()
    for wait in pending:
        wait()


def reduce_and_step(n, gathered, terms, weights, m, v):
    layers = m[0].shape[0]
    count = len(terms)
    chunks = count * layers
    pieces = [(layers, 2, one.shape[1] // 2, one.shape[2]) for one in m]
    blocks = [jax.ShapeDtypeStruct(one.shape, BF16) for one in m]
    new = []
    for w, piece, whole in zip(weights, pieces, gathered, strict=True):
        new += [jax.ShapeDtypeStruct(w.shape, BF16)] if whole else [jax.ShapeDtypeStruct(piece[2:], BF16)] * (2 * layers)
    out_shape = blocks + new
    sems = [pltpu.SemaphoreType.DMA((chunks, 2, 2) if name in BOTH_WAYS else (chunks, 2)) for name in SEMAPHORES]
    return pl.pallas_call(
        functools.partial(kernel, n, layers, gathered),
        out_shape=out_shape,
        in_specs=[pl.BlockSpec(memory_space=pl.ANY)] * (4 * count),
        out_specs=[pl.BlockSpec(memory_space=pl.ANY)] * len(out_shape),
        scratch_shapes=[pltpu.VMEM(p, BF16) for _ in range(6) for p in pieces]
        + [pltpu.VMEM(p[1:], F32) for _ in range(2) for p in pieces]
        + sems,
        compiler_params=pltpu.CompilerParams(collective_id=0, has_side_effects=True, vmem_limit_bytes=66_000_000),
        name="reduce_and_step",
    )(*terms, *weights, *m, *v)


def place_kernel(n, spots, *refs):
    pieces = refs[: len(spots)]
    out, buf, in_sem, out_sem = refs[len(spots) :]
    me = lax.axis_index("dp")
    half = buf.shape[1]
    loads = []
    for i, piece in enumerate(pieces):
        copy = pltpu.make_async_copy(piece, buf.at[i], in_sem.at[i])
        copy.start()
        loads.append(copy)
    stores = []
    for i, (layer, side, offset) in enumerate(spots):
        loads[i].wait()
        row = pl.multiple_of((2 * lax.rem(me + offset, n) + side) * half, 16)
        copy = pltpu.make_async_copy(buf.at[i], out.at[layer, pl.ds(row, half)], out_sem.at[i])
        copy.start()
        stores.append(copy)
    for copy in stores:
        copy.wait()


def place(n, shape, pieces):
    spots = tuple(pieces)
    piece = pieces[spots[0]]
    moved = 2 * len(spots) * piece.size * 2
    return pl.pallas_call(
        functools.partial(place_kernel, n, spots),
        out_shape=jax.ShapeDtypeStruct(shape, BF16),
        in_specs=[pl.BlockSpec(memory_space=pl.ANY)] * len(spots),
        out_specs=pl.BlockSpec(memory_space=pl.ANY),
        scratch_shapes=[pltpu.VMEM((len(spots), *piece.shape), BF16)] + [pltpu.SemaphoreType.DMA((len(spots),))] * 2,
        cost_estimate=pl.CostEstimate(flops=moved, bytes_accessed=moved, transcendentals=0),
        name="place",
    )(*pieces.values())


def finish_kernel(g, m, v, *refs):
    m_out, v_out = refs[-2:]
    m_out[...], v_out[...] = moments(m[...], v[...], g[...].astype(F32))
    if len(refs) > 2:
        w, w_out = refs[:2]
        w_out[...] = w[...]


def finish(g, m, v, *w):
    layers, depth, width = m.shape
    steps = next(k for k in range(7, 0, -1) if depth % (16 * k) == 0)
    block = pl.BlockSpec((1, depth // steps, width), lambda l, i: (l, i, 0))
    whole = [pl.BlockSpec((1, one.shape[1] // steps, width), lambda l, i: (l, i, 0)) for one in w]
    moved = m.size * 18 + sum(one.size * 4 for one in w)
    return pl.pallas_call(
        finish_kernel,
        grid=(layers, steps),
        out_shape=[jax.ShapeDtypeStruct(one.shape, BF16) for one in w] + [jax.ShapeDtypeStruct(m.shape, F32)] * 2,
        in_specs=[block] * 3 + whole,
        out_specs=whole + [block] * 2,
        cost_estimate=pl.CostEstimate(flops=moved, bytes_accessed=moved, transcendentals=0),
    )(g, m, v, *w)


def gather(n, shape, own):
    right, left = ([(i, (i + way) % n) for i in range(n)] for way in (1, n - 1))
    near, far = {}, {}
    for layer, sides in enumerate(own):
        for side, ahead in enumerate((right, left)):
            near[layer, side, 0] = sides[side]
            near[layer, side, (n - 1, 1)[side]] = lax.ppermute(sides[side], "dp", ahead)
        for side, behind in enumerate((left, right)):
            near[layer, side, (1, n - 1)[side]] = lax.ppermute(sides[side], "dp", behind)
    for layer, sides in enumerate(own):
        for side, ahead in enumerate((right, left)):
            far[layer, side] = lax.ppermute(near[layer, side, (n - 1, 1)[side]], "dp", ahead)
    whole = place(n, shape, near)
    opposite = lax.rem(lax.axis_index("dp") + 2, n)
    for (layer, side), piece in far.items():
        whole = lax.dynamic_update_slice(whole, piece[None], (layer, (2 * opposite + side) * piece.shape[0], 0))
    return whole


GATHERED = (True, True, False)


def solution(mesh):
    n = mesh.shape["dp"]

    def inner(*arrays):
        terms, weights, m, v = (arrays[i : i + 3] for i in (0, 3, 6, 9))
        layers = m[0].shape[0]
        out = list(reduce_and_step(n, GATHERED, terms, weights, m, v))
        sums = [out.pop(0) for _ in range(3)]
        new, m_new, v_new = [], [], []
        for k, whole in enumerate(GATHERED):
            held = [out.pop(0)] if whole else []
            *w, a, b = finish(sums[k], m[k], v[k], *held)
            new.append(w[0] if whole else gather(n, weights[k].shape, [[out.pop(0) for _ in range(2)] for _ in range(layers)]))
            m_new.append(a)
            v_new.append(b)
        return (*new, *m_new, *v_new)

    all_of, cut = P(None, None, None), P(None, "dp", None)
    return jax.shard_map(
        inner,
        mesh=mesh,
        in_specs=(P(("rep", "dp"), None, None, None),) * 3 + (all_of,) * 3 + (cut,) * 6,
        out_specs=(P("rep", None, None),) * 3 + (P("rep", "dp", None),) * 6,
        check_vma=False,
    )
```

```python
import functools

import jax
import jax.numpy as jnp
from jax import lax
from jax.experimental import pallas as pl
from jax.experimental.pallas import tpu as pltpu
from jax.sharding import PartitionSpec as P


MESH = pl.DeviceIdType.MESH
BF16, F32 = jnp.bfloat16, jnp.float32
SENT = ("far_s", "far_r", "rel_s", "rel_r", "dir_s", "dir_r", "fwd_s", "fwd_r")
LOCAL = ("term", "own", "w", "m", "v", "g_out", "w_out")
BOTH_WAYS = ("near_s", "near_r")
SEMAPHORES = (*SENT, *LOCAL, *BOTH_WAYS, "again")
LATER = 7


def moments(m, v, g):
    return 0.9 * m + 0.1 * g, 0.95 * v + 0.05 * g * g


def weight(w, m, v):
    return w - 0.02 * (m * lax.rsqrt(v + 1e-8) + 0.1 * w)


def columns(width):
    parts = -(-width // 1024)
    while width % (parts * 128):
        parts += 1
    return [slice(i * (width // parts), (i + 1) * (width // parts)) for i in range(parts)]


def tiled(shape, body):
    def row(i, carry):
        rows = pl.ds(pl.multiple_of(i * 16, 16), 16)
        for cols in columns(shape[1]):
            body(rows, cols)
        return carry

    lax.fori_loop(0, shape[0] // 16, row, 0)


def kernel(n, layers, gathered, *refs):
    count = len(gathered)
    refs = list(refs)
    take = lambda k: [refs.pop(0) for _ in range(k)]
    g, w, m, v = take(count), take(count), take(count), take(count)
    g_out = take(count)
    w_out = [take(1)[0] if whole else [[refs.pop(0) for _ in range(2)] for _ in range(layers)] for whole in gathered]
    far, rel, direct, term, own, new = (take(count) for _ in range(6))
    m_buf, v_buf = take(count), take(count)
    sem = dict(zip(SEMAPHORES, refs, strict=True))

    me = lax.axis_index("dp")
    right, left = lax.rem(me + 1, n), lax.rem(me + n - 1, n)
    opposite = lax.rem(me + 2, n)
    ahead, behind = (right, left), (left, right)

    barrier = pltpu.get_barrier_semaphore()
    for peer in (left, right):
        pl.semaphore_signal(barrier, inc=1, device_id={"dp": peer}, device_id_type=MESH)
    pl.semaphore_wait(barrier, 2)
    late = lax.rem(lax.axis_index("rep"), 2)

    def again(i, carry):
        for peer in (left, right):
            pl.semaphore_signal(sem["again"].at[lax.rem(i, 2)], inc=1, device_id={"dp": peer}, device_id_type=MESH)
        pl.semaphore_wait(sem["again"].at[lax.rem(i, 2)], 2)
        return carry

    lax.fori_loop(0, LATER * late, again, 0)

    chunks = [(k, layer) for k in range(count) for layer in range(layers)]
    pending = []

    def rows(k, block, side):
        half = far[k].shape[2]
        return pl.ds(pl.multiple_of((2 * block + side) * half, 16), half)

    def send(src, dst, send_sem, recv_sem, peer):
        copy = pltpu.make_async_remote_copy(src, dst, send_sem, recv_sem, device_id={"dp": peer}, device_id_type=MESH)
        copy.start()
        pending.append(copy.wait_send)
        return copy

    def local(src, dst, s):
        copy = pltpu.make_async_copy(src, dst, s)
        copy.start()
        return copy

    sent, loads, steps = {}, {}, {}

    def first(c):
        k, l = chunks[c]
        for side in (0, 1):
            sent["far", c, side] = send(
                g[k].at[0, l, rows(k, opposite, side)], far[k].at[l, side], sem["far_s"].at[c, side], sem["far_r"].at[c, side], ahead[side]
            )
        for side in (0, 1):
            sent["dir", c, side] = send(
                g[k].at[0, l, rows(k, behind[side], side)], direct[k].at[l, side], sem["dir_s"].at[c, side], sem["dir_r"].at[c, side], behind[side]
            )
        for side in (0, 1):
            loads["term", c, side] = local(g[k].at[0, l, rows(k, ahead[side], side)], term[k].at[l, side], sem["term"].at[c, side])
        for side in (0, 1):
            loads["own", c, side] = local(g[k].at[0, l, rows(k, me, side)], own[k].at[l, side], sem["own"].at[c, side])
            loads["w", c, side] = local(w[k].at[l, rows(k, me, side)], new[k].at[l, side], sem["w"].at[c, side])

    def load_moments(c, side):
        k, l = chunks[c]
        half = far[k].shape[2]
        here = pl.ds(side * half, half)
        steps[c, side] = (
            local(m[k].at[l, here], m_buf[k].at[side], sem["m"].at[c, side]),
            local(v[k].at[l, here], v_buf[k].at[side], sem["v"].at[c, side]),
        )

    def relay(c):
        k, l = chunks[c]
        for side in (0, 1):
            sent["far", c, side].wait_recv()
            loads["term", c, side].wait()
            sums, mine = far[k].at[l, side], term[k].at[l, side]

            def add(r, cols):
                sums[r, cols] = (sums[r, cols].astype(F32) + mine[r, cols].astype(F32)).astype(BF16)

            tiled(sums.shape, add)
            sent["rel", c, side] = send(sums, rel[k].at[l, side], sem["rel_s"].at[c, side], sem["rel_r"].at[c, side], ahead[side])

    def step(c):
        k, l = chunks[c]
        half = far[k].shape[2]
        for side in (0, 1):
            sent["dir", c, side].wait_recv()
            sent["rel", c, side].wait_recv()
            loads["own", c, side].wait()
            loads["w", c, side].wait()
            for load in steps[c, side]:
                load.wait()
            a, b, o, x = (array[k].at[l, side] for array in (rel, direct, own, new))
            ms, vs = m_buf[k].at[side], v_buf[k].at[side]

            def update(r, cols):
                total = (a[r, cols].astype(F32) + b[r, cols].astype(F32) + o[r, cols].astype(F32)).astype(BF16)
                o[r, cols] = total
                m_new, v_new = moments(ms[r, cols], vs[r, cols], total.astype(F32))
                x[r, cols] = weight(x[r, cols].astype(F32), m_new, v_new).astype(BF16)

            tiled(o.shape, update)
            here = pl.ds(side * half, half)
            pending.append(local(o, g_out[k].at[l, here], sem["g_out"].at[c, side]).wait)
            if gathered[k]:
                place = w_out[k].at[l, rows(k, me, side)]
                for way, peer in enumerate((ahead[side], behind[side])):
                    sent["near", c, side, way] = send(x, place, sem["near_s"].at[c, side, way], sem["near_r"].at[c, side, way], peer)
            else:
                place = w_out[k][l][side]
            pending.append(local(x, place, sem["w_out"].at[c, side]).wait)
            if c + 1 < len(chunks):
                load_moments(c + 1, side)

    def forward(c):
        k, l = chunks[c]
        if not gathered[k]:
            return
        for side in (0, 1):
            sent["near", c, side, 0].wait_recv()
            place = w_out[k].at[l, rows(k, behind[side], side)]
            sent["fwd", c, side] = send(place, place, sem["fwd_s"].at[c, side], sem["fwd_r"].at[c, side], ahead[side])

    last = len(chunks)
    for c in range(min(2, last)):
        first(c)
    for side in (0, 1):
        load_moments(0, side)
    for c in range(last + 2):
        if c + 2 < last:
            first(c + 2)
        if c < last:
            relay(c)
        if 0 <= c - 1 < last:
            step(c - 1)
        if 0 <= c - 2 < last:
            forward(c - 2)
    for key, copy in sent.items():
        if key[0] == "fwd" or (key[0] == "near" and key[3] == 1):
            copy.wait_recv()
    for wait in pending:
        wait()


def reduce_and_step(n, gathered, terms, weights, m, v):
    layers = m[0].shape[0]
    count = len(terms)
    chunks = count * layers
    pieces = [(layers, 2, one.shape[1] // 2, one.shape[2]) for one in m]
    blocks = [jax.ShapeDtypeStruct(one.shape, BF16) for one in m]
    new = []
    for w, piece, whole in zip(weights, pieces, gathered, strict=True):
        new += [jax.ShapeDtypeStruct(w.shape, BF16)] if whole else [jax.ShapeDtypeStruct(piece[2:], BF16)] * (2 * layers)
    out_shape = blocks + new
    sems = [pltpu.SemaphoreType.DMA((chunks, 2, 2) if name in BOTH_WAYS else (chunks, 2)) for name in SEMAPHORES[:-1]]
    sems.append(pltpu.SemaphoreType.REGULAR((2,)))
    return pl.pallas_call(
        functools.partial(kernel, n, layers, gathered),
        out_shape=out_shape,
        in_specs=[pl.BlockSpec(memory_space=pl.ANY)] * (4 * count),
        out_specs=[pl.BlockSpec(memory_space=pl.ANY)] * len(out_shape),
        scratch_shapes=[pltpu.VMEM(p, BF16) for _ in range(6) for p in pieces]
        + [pltpu.VMEM(p[1:], F32) for _ in range(2) for p in pieces]
        + sems,
        compiler_params=pltpu.CompilerParams(collective_id=0, has_side_effects=True, vmem_limit_bytes=66_000_000),
        name="reduce_and_step",
    )(*terms, *weights, *m, *v)


def place_kernel(n, spots, *refs):
    pieces = refs[: len(spots)]
    out, buf, in_sem, out_sem = refs[len(spots) :]
    me = lax.axis_index("dp")
    half = buf.shape[1]
    loads = []
    for i, piece in enumerate(pieces):
        copy = pltpu.make_async_copy(piece, buf.at[i], in_sem.at[i])
        copy.start()
        loads.append(copy)
    stores = []
    for i, (layer, side, offset) in enumerate(spots):
        loads[i].wait()
        row = pl.multiple_of((2 * lax.rem(me + offset, n) + side) * half, 16)
        copy = pltpu.make_async_copy(buf.at[i], out.at[layer, pl.ds(row, half)], out_sem.at[i])
        copy.start()
        stores.append(copy)
    for copy in stores:
        copy.wait()


def place(n, shape, pieces):
    spots = tuple(pieces)
    piece = pieces[spots[0]]
    moved = 2 * len(spots) * piece.size * 2
    return pl.pallas_call(
        functools.partial(place_kernel, n, spots),
        out_shape=jax.ShapeDtypeStruct(shape, BF16),
        in_specs=[pl.BlockSpec(memory_space=pl.ANY)] * len(spots),
        out_specs=pl.BlockSpec(memory_space=pl.ANY),
        scratch_shapes=[pltpu.VMEM((len(spots), *piece.shape), BF16)] + [pltpu.SemaphoreType.DMA((len(spots),))] * 2,
        cost_estimate=pl.CostEstimate(flops=moved, bytes_accessed=moved, transcendentals=0),
        name="place",
    )(*pieces.values())


def carry_kernel(parts, src, out, buf, in_sem, out_sem):
    layers, depth, _ = src.shape
    spots = [(l, pl.ds(i * (depth // parts), depth // parts)) for l in range(layers) for i in range(parts)]
    loads = [pltpu.make_async_copy(src.at[l, rows], buf.at[l, rows], in_sem.at[i]) for i, (l, rows) in enumerate(spots)]
    stores = [pltpu.make_async_copy(buf.at[l, rows], out.at[l, rows], out_sem.at[i]) for i, (l, rows) in enumerate(spots)]
    for load in loads:
        load.start()
    for load, store in zip(loads, stores, strict=True):
        load.wait()
        store.start()
    for store in stores:
        store.wait()


def carry(w):
    parts = next(k for k in range(8, 0, -1) if w.shape[1] % (16 * k) == 0)
    moved = 4 * w.size
    return pl.pallas_call(
        functools.partial(carry_kernel, parts),
        out_shape=jax.ShapeDtypeStruct(w.shape, w.dtype),
        in_specs=[pl.BlockSpec(memory_space=pl.ANY)],
        out_specs=pl.BlockSpec(memory_space=pl.ANY),
        scratch_shapes=[pltpu.VMEM(w.shape, w.dtype)] + [pltpu.SemaphoreType.DMA((w.shape[0] * parts,))] * 2,
        cost_estimate=pl.CostEstimate(flops=moved, bytes_accessed=moved, transcendentals=0),
    )(w)


def gather(n, shape, own):
    right, left = ([(i, (i + way) % n) for i in range(n)] for way in (1, n - 1))
    near, far = {}, {}
    for layer, sides in enumerate(own):
        for side, ahead in enumerate((right, left)):
            near[layer, side, 0] = sides[side]
            near[layer, side, (n - 1, 1)[side]] = lax.ppermute(sides[side], "dp", ahead)
        for side, behind in enumerate((left, right)):
            near[layer, side, (1, n - 1)[side]] = lax.ppermute(sides[side], "dp", behind)
    for layer, sides in enumerate(own):
        for side, ahead in enumerate((right, left)):
            far[layer, side] = lax.ppermute(near[layer, side, (n - 1, 1)[side]], "dp", ahead)
    whole = place(n, shape, near)
    opposite = lax.rem(lax.axis_index("dp") + 2, n)
    for (layer, side), piece in far.items():
        whole = lax.dynamic_update_slice(whole, piece[None], (layer, (2 * opposite + side) * piece.shape[0], 0))
    return whole


GATHERED = (True, True, False)


def solution(mesh):
    n = mesh.shape["dp"]

    def inner(*arrays):
        terms, weights, m, v = (arrays[i : i + 3] for i in (0, 3, 6, 9))
        layers = m[0].shape[0]
        out = list(reduce_and_step(n, GATHERED, terms, weights, m, v))
        sums = [out.pop(0) for _ in range(3)]
        new, pairs = [], []
        for k, whole in enumerate(GATHERED):
            pairs.append(moments(m[k], v[k], sums[k].astype(F32)))
            if whole:
                new.append(carry(out.pop(0)))
            else:
                new.append(gather(n, weights[k].shape, [[out.pop(0) for _ in range(2)] for _ in range(layers)]))
        return (*new, *(one[0] for one in pairs), *(one[1] for one in pairs))

    all_of, cut = P(None, None, None), P(None, "dp", None)
    return jax.shard_map(
        inner,
        mesh=mesh,
        in_specs=(P(("rep", "dp"), None, None, None),) * 3 + (all_of,) * 3 + (cut,) * 6,
        out_specs=(P("rep", None, None),) * 3 + (P("rep", "dp", None),) * 6,
        check_vma=False,
    )
```

```python
import functools

import jax
import jax.numpy as jnp
from jax import lax
from jax.experimental import pallas as pl
from jax.experimental.pallas import tpu as pltpu
from jax.sharding import PartitionSpec as P


MESH = pl.DeviceIdType.MESH
BF16, F32 = jnp.bfloat16, jnp.float32
SENT = ("far_s", "far_r", "rel_s", "rel_r", "dir_s", "dir_r", "fwd_s", "fwd_r")
LOCAL = ("term", "own", "w", "m", "v", "g_out", "w_out")
BOTH_WAYS = ("near_s", "near_r")
SEMAPHORES = (*SENT, *LOCAL, *BOTH_WAYS, "again")
LATER = 6


def moments(m, v, g):
    return 0.9 * m + 0.1 * g, 0.95 * v + 0.05 * g * g


def weight(w, m, v):
    return w - 0.02 * (m * lax.rsqrt(v + 1e-8) + 0.1 * w)


def columns(width):
    parts = -(-width // 1024)
    while width % (parts * 128):
        parts += 1
    return [slice(i * (width // parts), (i + 1) * (width // parts)) for i in range(parts)]


def tiled(shape, body):
    def row(i, carry):
        rows = pl.ds(pl.multiple_of(i * 16, 16), 16)
        for cols in columns(shape[1]):
            body(rows, cols)
        return carry

    lax.fori_loop(0, shape[0] // 16, row, 0)


def kernel(n, layers, gathered, *refs):
    count = len(gathered)
    refs = list(refs)
    take = lambda k: [refs.pop(0) for _ in range(k)]
    g, w, m, v = take(count), take(count), take(count), take(count)
    g_out = take(count)
    w_out = [take(1)[0] if whole else [[refs.pop(0) for _ in range(2)] for _ in range(layers)] for whole in gathered]
    far, rel, direct, term, own, new = (take(count) for _ in range(6))
    m_buf, v_buf = take(count), take(count)
    sem = dict(zip(SEMAPHORES, refs, strict=True))

    me = lax.axis_index("dp")
    right, left = lax.rem(me + 1, n), lax.rem(me + n - 1, n)
    opposite = lax.rem(me + 2, n)
    ahead, behind = (right, left), (left, right)

    barrier = pltpu.get_barrier_semaphore()
    for peer in (left, right):
        pl.semaphore_signal(barrier, inc=1, device_id={"dp": peer}, device_id_type=MESH)
    pl.semaphore_wait(barrier, 2)
    late = 1 - lax.rem(lax.axis_index("rep"), 2)

    def again(i, carry):
        for peer in (left, right):
            pl.semaphore_signal(sem["again"].at[lax.rem(i, 2)], inc=1, device_id={"dp": peer}, device_id_type=MESH)
        pl.semaphore_wait(sem["again"].at[lax.rem(i, 2)], 2)
        return carry

    lax.fori_loop(0, LATER * late, again, 0)

    chunks = [(k, layer) for k in range(count) for layer in range(layers)]
    pending = []

    def rows(k, block, side):
        half = far[k].shape[2]
        return pl.ds(pl.multiple_of((2 * block + side) * half, 16), half)

    def send(src, dst, send_sem, recv_sem, peer):
        copy = pltpu.make_async_remote_copy(src, dst, send_sem, recv_sem, device_id={"dp": peer}, device_id_type=MESH)
        copy.start()
        pending.append(copy.wait_send)
        return copy

    def local(src, dst, s):
        copy = pltpu.make_async_copy(src, dst, s)
        copy.start()
        return copy

    sent, loads, steps = {}, {}, {}

    def first(c):
        k, l = chunks[c]
        for side in (0, 1):
            sent["far", c, side] = send(
                g[k].at[0, l, rows(k, opposite, side)], far[k].at[l, side], sem["far_s"].at[c, side], sem["far_r"].at[c, side], ahead[side]
            )
        for side in (0, 1):
            sent["dir", c, side] = send(
                g[k].at[0, l, rows(k, behind[side], side)], direct[k].at[l, side], sem["dir_s"].at[c, side], sem["dir_r"].at[c, side], behind[side]
            )
        for side in (0, 1):
            loads["term", c, side] = local(g[k].at[0, l, rows(k, ahead[side], side)], term[k].at[l, side], sem["term"].at[c, side])
        for side in (0, 1):
            loads["own", c, side] = local(g[k].at[0, l, rows(k, me, side)], own[k].at[l, side], sem["own"].at[c, side])
            loads["w", c, side] = local(w[k].at[l, rows(k, me, side)], new[k].at[l, side], sem["w"].at[c, side])

    def load_moments(c, side):
        k, l = chunks[c]
        half = far[k].shape[2]
        here = pl.ds(side * half, half)
        steps[c, side] = (
            local(m[k].at[l, here], m_buf[k].at[side], sem["m"].at[c, side]),
            local(v[k].at[l, here], v_buf[k].at[side], sem["v"].at[c, side]),
        )

    def relay(c):
        k, l = chunks[c]
        for side in (0, 1):
            sent["far", c, side].wait_recv()
            loads["term", c, side].wait()
            sums, mine = far[k].at[l, side], term[k].at[l, side]

            def add(r, cols):
                sums[r, cols] = (sums[r, cols].astype(F32) + mine[r, cols].astype(F32)).astype(BF16)

            tiled(sums.shape, add)
            sent["rel", c, side] = send(sums, rel[k].at[l, side], sem["rel_s"].at[c, side], sem["rel_r"].at[c, side], ahead[side])

    def step(c):
        k, l = chunks[c]
        half = far[k].shape[2]
        for side in (0, 1):
            sent["dir", c, side].wait_recv()
            sent["rel", c, side].wait_recv()
            loads["own", c, side].wait()
            loads["w", c, side].wait()
            for load in steps[c, side]:
                load.wait()
            a, b, o, x = (array[k].at[l, side] for array in (rel, direct, own, new))
            ms, vs = m_buf[k].at[side], v_buf[k].at[side]

            def update(r, cols):
                total = (a[r, cols].astype(F32) + b[r, cols].astype(F32) + o[r, cols].astype(F32)).astype(BF16)
                o[r, cols] = total
                m_new, v_new = moments(ms[r, cols], vs[r, cols], total.astype(F32))
                x[r, cols] = weight(x[r, cols].astype(F32), m_new, v_new).astype(BF16)

            tiled(o.shape, update)
            here = pl.ds(side * half, half)
            pending.append(local(o, g_out[k].at[l, here], sem["g_out"].at[c, side]).wait)
            if gathered[k]:
                place = w_out[k].at[l, rows(k, me, side)]
                for way, peer in enumerate((ahead[side], behind[side])):
                    sent["near", c, side, way] = send(x, place, sem["near_s"].at[c, side, way], sem["near_r"].at[c, side, way], peer)
            else:
                place = w_out[k][l][side]
            pending.append(local(x, place, sem["w_out"].at[c, side]).wait)
            if c + 1 < len(chunks):
                load_moments(c + 1, side)

    def forward(c):
        k, l = chunks[c]
        if not gathered[k]:
            return
        for side in (0, 1):
            sent["near", c, side, 0].wait_recv()
            place = w_out[k].at[l, rows(k, behind[side], side)]
            sent["fwd", c, side] = send(place, place, sem["fwd_s"].at[c, side], sem["fwd_r"].at[c, side], ahead[side])

    last = len(chunks)
    for c in range(min(2, last)):
        first(c)
    for side in (0, 1):
        load_moments(0, side)
    for c in range(last + 2):
        if c + 2 < last:
            first(c + 2)
        if c < last:
            relay(c)
        if 0 <= c - 1 < last:
            step(c - 1)
        if 0 <= c - 2 < last:
            forward(c - 2)
    for key, copy in sent.items():
        if key[0] == "fwd" or (key[0] == "near" and key[3] == 1):
            copy.wait_recv()
    for wait in pending:
        wait()


def reduce_and_step(n, gathered, terms, weights, m, v):
    layers = m[0].shape[0]
    count = len(terms)
    chunks = count * layers
    pieces = [(layers, 2, one.shape[1] // 2, one.shape[2]) for one in m]
    blocks = [jax.ShapeDtypeStruct(one.shape, BF16) for one in m]
    new = []
    for w, piece, whole in zip(weights, pieces, gathered, strict=True):
        new += [jax.ShapeDtypeStruct(w.shape, BF16)] if whole else [jax.ShapeDtypeStruct(piece[2:], BF16)] * (2 * layers)
    out_shape = blocks + new
    sems = [pltpu.SemaphoreType.DMA((chunks, 2, 2) if name in BOTH_WAYS else (chunks, 2)) for name in SEMAPHORES[:-1]]
    sems.append(pltpu.SemaphoreType.REGULAR((2,)))
    return pl.pallas_call(
        functools.partial(kernel, n, layers, gathered),
        out_shape=out_shape,
        in_specs=[pl.BlockSpec(memory_space=pl.ANY)] * (4 * count),
        out_specs=[pl.BlockSpec(memory_space=pl.ANY)] * len(out_shape),
        scratch_shapes=[pltpu.VMEM(p, BF16) for _ in range(6) for p in pieces]
        + [pltpu.VMEM(p[1:], F32) for _ in range(2) for p in pieces]
        + sems,
        compiler_params=pltpu.CompilerParams(collective_id=0, has_side_effects=True, vmem_limit_bytes=66_000_000),
        name="reduce_and_step",
    )(*terms, *weights, *m, *v)


def place_kernel(n, spots, *refs):
    pieces = refs[: len(spots)]
    out, buf, in_sem, out_sem = refs[len(spots) :]
    me = lax.axis_index("dp")
    half = buf.shape[1]
    loads = []
    for i, piece in enumerate(pieces):
        copy = pltpu.make_async_copy(piece, buf.at[i], in_sem.at[i])
        copy.start()
        loads.append(copy)
    stores = []
    for i, (layer, side, offset) in enumerate(spots):
        loads[i].wait()
        row = pl.multiple_of((2 * lax.rem(me + offset, n) + side) * half, 16)
        copy = pltpu.make_async_copy(buf.at[i], out.at[layer, pl.ds(row, half)], out_sem.at[i])
        copy.start()
        stores.append(copy)
    for copy in stores:
        copy.wait()


def place(n, shape, pieces):
    spots = tuple(pieces)
    piece = pieces[spots[0]]
    moved = 2 * len(spots) * piece.size * 2
    return pl.pallas_call(
        functools.partial(place_kernel, n, spots),
        out_shape=jax.ShapeDtypeStruct(shape, BF16),
        in_specs=[pl.BlockSpec(memory_space=pl.ANY)] * len(spots),
        out_specs=pl.BlockSpec(memory_space=pl.ANY),
        scratch_shapes=[pltpu.VMEM((len(spots), *piece.shape), BF16)] + [pltpu.SemaphoreType.DMA((len(spots),))] * 2,
        cost_estimate=pl.CostEstimate(flops=moved, bytes_accessed=moved, transcendentals=0),
        name="place",
    )(*pieces.values())


def carry_kernel(parts, *refs):
    count = (len(refs) - 2) // 3
    src, out, buf = (refs[i * count : (i + 1) * count] for i in range(3))
    in_sem, out_sem = refs[3 * count :]
    layers, depth, _ = src[0].shape
    rows = depth // parts
    spots = [(k, l, pl.ds(i * rows, rows)) for k in range(count) for l in range(layers) for i in range(parts)]
    loads = [pltpu.make_async_copy(src[k].at[l, here], buf[k].at[l, here], in_sem.at[i]) for i, (k, l, here) in enumerate(spots)]
    stores = [pltpu.make_async_copy(buf[k].at[l, here], out[k].at[l, here], out_sem.at[i]) for i, (k, l, here) in enumerate(spots)]
    for load in loads:
        load.start()
    for load, store in zip(loads, stores, strict=True):
        load.wait()
        store.start()
    for store in stores:
        store.wait()


def carry(arrays):
    w, count = arrays[0], len(arrays)
    parts = next(k for k in range(8, 0, -1) if w.shape[1] % (16 * k) == 0)
    moved = 4 * w.size * count
    return pl.pallas_call(
        functools.partial(carry_kernel, parts),
        out_shape=[jax.ShapeDtypeStruct(w.shape, w.dtype)] * count,
        in_specs=[pl.BlockSpec(memory_space=pl.ANY)] * count,
        out_specs=[pl.BlockSpec(memory_space=pl.ANY)] * count,
        scratch_shapes=[pltpu.VMEM(w.shape, w.dtype)] * count + [pltpu.SemaphoreType.DMA((count * w.shape[0] * parts,))] * 2,
        cost_estimate=pl.CostEstimate(flops=moved, bytes_accessed=moved, transcendentals=0),
        name="carry",
    )(*arrays)


def gather(n, shape, own):
    right, left = ([(i, (i + way) % n) for i in range(n)] for way in (1, n - 1))
    near, far = {}, {}
    for layer, sides in enumerate(own):
        for side, ahead in enumerate((right, left)):
            near[layer, side, 0] = sides[side]
            near[layer, side, (n - 1, 1)[side]] = lax.ppermute(sides[side], "dp", ahead)
        for side, behind in enumerate((left, right)):
            near[layer, side, (1, n - 1)[side]] = lax.ppermute(sides[side], "dp", behind)
    for layer, sides in enumerate(own):
        for side, ahead in enumerate((right, left)):
            far[layer, side] = lax.ppermute(near[layer, side, (n - 1, 1)[side]], "dp", ahead)
    early = {(layer, side, 2): far[layer, side] for layer in range(len(own) - 1) for side in (0, 1)}
    whole = place(n, shape, {**near, **early})
    opposite = lax.rem(lax.axis_index("dp") + 2, n)
    for side in (0, 1):
        piece = far[len(own) - 1, side]
        whole = lax.dynamic_update_slice(whole, piece[None], (len(own) - 1, (2 * opposite + side) * piece.shape[0], 0))
    return whole


GATHERED = (True, True, False)


def solution(mesh):
    n = mesh.shape["dp"]

    def inner(*arrays):
        terms, weights, m, v = (arrays[i : i + 3] for i in (0, 3, 6, 9))
        layers = m[0].shape[0]
        out = list(reduce_and_step(n, GATHERED, terms, weights, m, v))
        sums = [out.pop(0) for _ in range(3)]
        held, new, pairs = [], [], []
        for k, whole in enumerate(GATHERED):
            pairs.append(moments(m[k], v[k], sums[k].astype(F32)))
            if whole:
                held.append(out.pop(0))
            else:
                new.append(gather(n, weights[k].shape, [[out.pop(0) for _ in range(2)] for _ in range(layers)]))
        new = [*carry(held), *new]
        return (*new, *(one[0] for one in pairs), *(one[1] for one in pairs))

    all_of, cut = P(None, None, None), P(None, "dp", None)
    return jax.shard_map(
        inner,
        mesh=mesh,
        in_specs=(P(("rep", "dp"), None, None, None),) * 3 + (all_of,) * 3 + (cut,) * 6,
        out_specs=(P("rep", None, None),) * 3 + (P("rep", "dp", None),) * 6,
        check_vma=False,
    )
```

```python
import functools

import jax
import jax.numpy as jnp
from jax import lax
from jax.experimental import pallas as pl
from jax.experimental.pallas import tpu as pltpu
from jax.sharding import PartitionSpec as P


MESH = pl.DeviceIdType.MESH
BF16, F32 = jnp.bfloat16, jnp.float32
SENT = ("far_s", "far_r", "rel_s", "rel_r", "dir_s", "dir_r", "fwd_s", "fwd_r")
LOCAL = ("term", "own", "w", "m", "v", "g_out")
BOTH_WAYS = ("near_s", "near_r", "w_out")
SEMAPHORES = (*SENT, *LOCAL, *BOTH_WAYS, "again")
LATER = 5


def moments(m, v, g):
    return 0.9 * m + 0.1 * g, 0.95 * v + 0.05 * g * g


def weight(w, m, v):
    return w - 0.02 * (m * lax.rsqrt(v + 1e-8) + 0.1 * w)


def columns(width):
    parts = -(-width // 1024)
    while width % (parts * 128):
        parts += 1
    return [slice(i * (width // parts), (i + 1) * (width // parts)) for i in range(parts)]


def cuts(half):
    last = max(16, half // 5 // 16 * 16)
    return (0, half - last), (half - last, last)


def tiled(shape, body):
    def row(i, carry):
        rows = pl.ds(pl.multiple_of(i * 16, 16), 16)
        for cols in columns(shape[1]):
            body(rows, cols)
        return carry

    lax.fori_loop(0, shape[0] // 16, row, 0)


def kernel(n, layers, gathered, *refs):
    count = len(gathered)
    refs = list(refs)
    take = lambda k: [refs.pop(0) for _ in range(k)]
    g, w, m, v = take(count), take(count), take(count), take(count)
    g_out = take(count)
    w_out = [take(1)[0] if whole else [take(2) for _ in cuts(w[k].shape[1] // (2 * n))] for k, whole in enumerate(gathered)]
    far, rel, direct, term, own, new = (take(count) for _ in range(6))
    m_buf, v_buf = take(count), take(count)
    sem = dict(zip(SEMAPHORES, refs, strict=True))

    me = lax.axis_index("dp")
    right, left = lax.rem(me + 1, n), lax.rem(me + n - 1, n)
    opposite = lax.rem(me + 2, n)
    ahead, behind = (right, left), (left, right)

    barrier = pltpu.get_barrier_semaphore()
    for peer in (left, right):
        pl.semaphore_signal(barrier, inc=1, device_id={"dp": peer}, device_id_type=MESH)
    pl.semaphore_wait(barrier, 2)
    late = 1 - lax.rem(lax.axis_index("rep"), 2)

    def again(i, carry):
        for peer in (left, right):
            pl.semaphore_signal(sem["again"].at[lax.rem(i, 2)], inc=1, device_id={"dp": peer}, device_id_type=MESH)
        pl.semaphore_wait(sem["again"].at[lax.rem(i, 2)], 2)
        return carry

    lax.fori_loop(0, LATER * late, again, 0)

    chunks = [(k, layer) for k in range(count) for layer in range(layers)]
    pending = []

    def rows(k, block, side):
        half = far[k].shape[2]
        return pl.ds(pl.multiple_of((2 * block + side) * half, 16), half)

    def send(src, dst, send_sem, recv_sem, peer):
        copy = pltpu.make_async_remote_copy(src, dst, send_sem, recv_sem, device_id={"dp": peer}, device_id_type=MESH)
        copy.start()
        pending.append(copy.wait_send)
        return copy

    def local(src, dst, s):
        copy = pltpu.make_async_copy(src, dst, s)
        copy.start()
        return copy

    sent, loads, steps = {}, {}, {}

    def first(c):
        k, l = chunks[c]
        for side in (0, 1):
            sent["far", c, side] = send(
                g[k].at[0, l, rows(k, opposite, side)], far[k].at[l, side], sem["far_s"].at[c, side], sem["far_r"].at[c, side], ahead[side]
            )
        for side in (0, 1):
            sent["dir", c, side] = send(
                g[k].at[0, l, rows(k, behind[side], side)], direct[k].at[l, side], sem["dir_s"].at[c, side], sem["dir_r"].at[c, side], behind[side]
            )
        for side in (0, 1):
            loads["term", c, side] = local(g[k].at[0, l, rows(k, ahead[side], side)], term[k].at[l, side], sem["term"].at[c, side])
        for side in (0, 1):
            loads["own", c, side] = local(g[k].at[0, l, rows(k, me, side)], own[k].at[l, side], sem["own"].at[c, side])
            loads["w", c, side] = local(w[k].at[l, rows(k, me, side)], new[k].at[l, side], sem["w"].at[c, side])

    def load_moments(c, side):
        k, l = chunks[c]
        half = far[k].shape[2]
        here = pl.ds(side * half, half)
        steps[c, side] = (
            local(m[k].at[l, here], m_buf[k].at[side], sem["m"].at[c, side]),
            local(v[k].at[l, here], v_buf[k].at[side], sem["v"].at[c, side]),
        )

    def relay(c):
        k, l = chunks[c]
        for side in (0, 1):
            sent["far", c, side].wait_recv()
            loads["term", c, side].wait()
            sums, mine = far[k].at[l, side], term[k].at[l, side]

            def add(r, cols):
                sums[r, cols] = (sums[r, cols].astype(F32) + mine[r, cols].astype(F32)).astype(BF16)

            tiled(sums.shape, add)
            sent["rel", c, side] = send(sums, rel[k].at[l, side], sem["rel_s"].at[c, side], sem["rel_r"].at[c, side], ahead[side])

    def step(c):
        k, l = chunks[c]
        half = far[k].shape[2]
        for side in (0, 1):
            sent["dir", c, side].wait_recv()
            sent["rel", c, side].wait_recv()
            loads["own", c, side].wait()
            loads["w", c, side].wait()
            for load in steps[c, side]:
                load.wait()
            a, b, o, x = (array[k].at[l, side] for array in (rel, direct, own, new))
            ms, vs = m_buf[k].at[side], v_buf[k].at[side]

            def update(r, cols):
                total = (a[r, cols].astype(F32) + b[r, cols].astype(F32) + o[r, cols].astype(F32)).astype(BF16)
                o[r, cols] = total
                m_new, v_new = moments(ms[r, cols], vs[r, cols], total.astype(F32))
                x[r, cols] = weight(x[r, cols].astype(F32), m_new, v_new).astype(BF16)

            tiled(o.shape, update)
            here = pl.ds(side * half, half)
            pending.append(local(o, g_out[k].at[l, here], sem["g_out"].at[c, side]).wait)
            if gathered[k]:
                place = w_out[k].at[l, rows(k, me, side)]
                for way, peer in enumerate((ahead[side], behind[side])):
                    sent["near", c, side, way] = send(x, place, sem["near_s"].at[c, side, way], sem["near_r"].at[c, side, way], peer)
                pending.append(local(x, place, sem["w_out"].at[c, side, 0]).wait)
            else:
                for i, (start, size) in enumerate(cuts(half)):
                    pending.append(local(x.at[pl.ds(start, size)], w_out[k][i][side].at[l], sem["w_out"].at[c, side, i]).wait)
            if c + 1 < len(chunks):
                load_moments(c + 1, side)

    def forward(c):
        k, l = chunks[c]
        if not gathered[k]:
            return
        for side in (0, 1):
            sent["near", c, side, 0].wait_recv()
            place = w_out[k].at[l, rows(k, behind[side], side)]
            sent["fwd", c, side] = send(place, place, sem["fwd_s"].at[c, side], sem["fwd_r"].at[c, side], ahead[side])

    last = len(chunks)
    for c in range(min(2, last)):
        first(c)
    for side in (0, 1):
        load_moments(0, side)
    for c in range(last + 2):
        if c + 2 < last:
            first(c + 2)
        if c < last:
            relay(c)
        if 0 <= c - 1 < last:
            step(c - 1)
        if 0 <= c - 2 < last:
            forward(c - 2)
    for key, copy in sent.items():
        if key[0] == "fwd" or (key[0] == "near" and key[3] == 1):
            copy.wait_recv()
    for wait in pending:
        wait()


def reduce_and_step(n, gathered, terms, weights, m, v):
    layers = m[0].shape[0]
    count = len(terms)
    chunks = count * layers
    pieces = [(layers, 2, one.shape[1] // 2, one.shape[2]) for one in m]
    blocks = [jax.ShapeDtypeStruct(one.shape, BF16) for one in m]
    new = []
    for w, piece, whole in zip(weights, pieces, gathered, strict=True):
        if whole:
            new.append(jax.ShapeDtypeStruct(w.shape, BF16))
        else:
            new += [jax.ShapeDtypeStruct((layers, size, piece[3]), BF16) for _, size in cuts(piece[2]) for _ in range(2)]
    out_shape = blocks + new
    sems = [pltpu.SemaphoreType.DMA((chunks, 2, 2) if name in BOTH_WAYS else (chunks, 2)) for name in SEMAPHORES[:-1]]
    sems.append(pltpu.SemaphoreType.REGULAR((2,)))
    return pl.pallas_call(
        functools.partial(kernel, n, layers, gathered),
        out_shape=out_shape,
        in_specs=[pl.BlockSpec(memory_space=pl.ANY)] * (4 * count),
        out_specs=[pl.BlockSpec(memory_space=pl.ANY)] * len(out_shape),
        scratch_shapes=[pltpu.VMEM(p, BF16) for _ in range(6) for p in pieces]
        + [pltpu.VMEM(p[1:], F32) for _ in range(2) for p in pieces]
        + sems,
        compiler_params=pltpu.CompilerParams(collective_id=0, has_side_effects=True, vmem_limit_bytes=66_000_000),
        name="reduce_and_step",
    )(*terms, *weights, *m, *v)


def place_kernel(n, spots, *refs):
    count = len(spots)
    pieces, out, bufs = refs[:count], refs[count], refs[count + 1 : 2 * count + 1]
    in_sem, out_sem = refs[2 * count + 1 :]
    me = lax.axis_index("dp")
    half = out.shape[1] // (2 * n)
    loads = []
    for i, piece in enumerate(pieces):
        copy = pltpu.make_async_copy(piece, bufs[i], in_sem.at[i])
        copy.start()
        loads.append(copy)
    stores = []
    for i, (start, side, offset) in enumerate(spots):
        loads[i].wait()
        row = pl.multiple_of((2 * lax.rem(me + offset, n) + side) * half + start, 16)
        copy = pltpu.make_async_copy(bufs[i], out.at[:, pl.ds(row, bufs[i].shape[1])], out_sem.at[i])
        copy.start()
        stores.append(copy)
    for copy in stores:
        copy.wait()


def place(n, shape, pieces):
    spots = tuple(pieces)
    moved = 4 * sum(piece.size for piece in pieces.values())
    return pl.pallas_call(
        functools.partial(place_kernel, n, spots),
        out_shape=jax.ShapeDtypeStruct(shape, BF16),
        in_specs=[pl.BlockSpec(memory_space=pl.ANY)] * len(spots),
        out_specs=pl.BlockSpec(memory_space=pl.ANY),
        scratch_shapes=[pltpu.VMEM(piece.shape, BF16) for piece in pieces.values()] + [pltpu.SemaphoreType.DMA((len(spots),))] * 2,
        cost_estimate=pl.CostEstimate(flops=moved, bytes_accessed=moved, transcendentals=0),
        name="place",
    )(*pieces.values())


def carry_kernel(parts, *refs):
    count = (len(refs) - 2) // 3
    src, out, buf = (refs[i * count : (i + 1) * count] for i in range(3))
    in_sem, out_sem = refs[3 * count :]
    layers, depth, _ = src[0].shape
    rows = depth // parts
    spots = [(k, l, pl.ds(i * rows, rows)) for k in range(count) for l in range(layers) for i in range(parts)]
    loads = [pltpu.make_async_copy(src[k].at[l, here], buf[k].at[l, here], in_sem.at[i]) for i, (k, l, here) in enumerate(spots)]
    stores = [pltpu.make_async_copy(buf[k].at[l, here], out[k].at[l, here], out_sem.at[i]) for i, (k, l, here) in enumerate(spots)]
    for load in loads:
        load.start()
    for load, store in zip(loads, stores, strict=True):
        load.wait()
        store.start()
    for store in stores:
        store.wait()


def carry(arrays):
    w, count = arrays[0], len(arrays)
    parts = next(k for k in range(8, 0, -1) if w.shape[1] % (16 * k) == 0)
    moved = 4 * w.size * count
    return pl.pallas_call(
        functools.partial(carry_kernel, parts),
        out_shape=[jax.ShapeDtypeStruct(w.shape, w.dtype)] * count,
        in_specs=[pl.BlockSpec(memory_space=pl.ANY)] * count,
        out_specs=[pl.BlockSpec(memory_space=pl.ANY)] * count,
        scratch_shapes=[pltpu.VMEM(w.shape, w.dtype)] * count + [pltpu.SemaphoreType.DMA((count * w.shape[0] * parts,))] * 2,
        cost_estimate=pl.CostEstimate(flops=moved, bytes_accessed=moved, transcendentals=0),
        name="carry",
    )(*arrays)


def gather(n, shape, own):
    half = shape[1] // (2 * n)
    right, left = ([(i, (i + way) % n) for i in range(n)] for way in (1, n - 1))
    near, far = {}, {}
    for i, (start, _) in enumerate(cuts(half)):
        for side, ahead in enumerate((right, left)):
            near[start, side, 0] = own[i][side]
            near[start, side, (n - 1, 1)[side]] = lax.ppermute(own[i][side], "dp", ahead)
        for side, behind in enumerate((left, right)):
            near[start, side, (1, n - 1)[side]] = lax.ppermute(own[i][side], "dp", behind)
    for start, _ in cuts(half):
        for side, ahead in enumerate((right, left)):
            far[start, side] = lax.ppermute(near[start, side, (n - 1, 1)[side]], "dp", ahead)
    whole = place(n, shape, near)
    opposite = lax.rem(lax.axis_index("dp") + 2, n)
    for (start, side), piece in far.items():
        whole = lax.dynamic_update_slice(whole, piece, (0, (2 * opposite + side) * half + start, 0))
    return whole


GATHERED = (True, True, False)


def solution(mesh):
    n = mesh.shape["dp"]

    def inner(*arrays):
        terms, weights, m, v = (arrays[i : i + 3] for i in (0, 3, 6, 9))
        out = list(reduce_and_step(n, GATHERED, terms, weights, m, v))
        sums = [out.pop(0) for _ in range(3)]
        held, new, pairs = [], [], []
        for k, whole in enumerate(GATHERED):
            pairs.append(moments(m[k], v[k], sums[k].astype(F32)))
            if whole:
                held.append(out.pop(0))
            else:
                new.append(gather(n, weights[k].shape, [[out.pop(0) for _ in range(2)] for _ in cuts(m[k].shape[1] // 2)]))
        new = [*carry(held), *new]
        return (*new, *(one[0] for one in pairs), *(one[1] for one in pairs))

    all_of, cut = P(None, None, None), P(None, "dp", None)
    return jax.shard_map(
        inner,
        mesh=mesh,
        in_specs=(P(("rep", "dp"), None, None, None),) * 3 + (all_of,) * 3 + (cut,) * 6,
        out_specs=(P("rep", None, None),) * 3 + (P("rep", "dp", None),) * 6,
        check_vma=False,
    )
```

```python
import functools

import jax
import jax.numpy as jnp
from jax import lax
from jax.experimental import pallas as pl
from jax.experimental.pallas import tpu as pltpu
from jax.sharding import PartitionSpec as P


MESH = pl.DeviceIdType.MESH
BF16, F32 = jnp.bfloat16, jnp.float32
SENT = ("far_s", "far_r", "rel_s", "rel_r", "dir_s", "dir_r", "fwd_s", "fwd_r")
LOCAL = ("term", "own", "w", "m", "v", "g_out")
BOTH_WAYS = ("near_s", "near_r", "w_out")
SEMAPHORES = (*SENT, *LOCAL, *BOTH_WAYS, "again")
LATER = 5


def moments(m, v, g):
    return 0.9 * m + 0.1 * g, 0.95 * v + 0.05 * g * g


def weight(w, m, v):
    return w - 0.02 * (m * lax.rsqrt(v + 1e-8) + 0.1 * w)


def columns(width):
    parts = -(-width // 1024)
    while width % (parts * 128):
        parts += 1
    return [slice(i * (width // parts), (i + 1) * (width // parts)) for i in range(parts)]


def cuts(half):
    last = max(16, half // 5 // 16 * 16)
    return (0, last, half - last), (half - last, 0, last)


def tiled(shape, body):
    def row(i, carry):
        rows = pl.ds(pl.multiple_of(i * 16, 16), 16)
        for cols in columns(shape[1]):
            body(rows, cols)
        return carry

    lax.fori_loop(0, shape[0] // 16, row, 0)


def kernel(n, layers, gathered, *refs):
    count = len(gathered)
    refs = list(refs)
    take = lambda k: [refs.pop(0) for _ in range(k)]
    g, w, m, v = take(count), take(count), take(count), take(count)
    g_out = take(count)
    w_out = [take(1)[0] if whole else [take(2) for _ in cuts(w[k].shape[1] // (2 * n))] for k, whole in enumerate(gathered)]
    far, rel, direct, term, own, new = (take(count) for _ in range(6))
    m_buf, v_buf = take(count), take(count)
    sem = dict(zip(SEMAPHORES, refs, strict=True))

    me = lax.axis_index("dp")
    right, left = lax.rem(me + 1, n), lax.rem(me + n - 1, n)
    opposite = lax.rem(me + 2, n)
    ahead, behind = (right, left), (left, right)

    barrier = pltpu.get_barrier_semaphore()
    for peer in (left, right):
        pl.semaphore_signal(barrier, inc=1, device_id={"dp": peer}, device_id_type=MESH)
    pl.semaphore_wait(barrier, 2)
    late = 1 - lax.rem(lax.axis_index("rep"), 2)

    def again(i, carry):
        for peer in (left, right):
            pl.semaphore_signal(sem["again"].at[lax.rem(i, 2)], inc=1, device_id={"dp": peer}, device_id_type=MESH)
        pl.semaphore_wait(sem["again"].at[lax.rem(i, 2)], 2)
        return carry

    lax.fori_loop(0, LATER * late, again, 0)

    chunks = [(k, layer) for k in range(count) for layer in range(layers)]
    pending = []

    def rows(k, block, side):
        half = far[k].shape[2]
        return pl.ds(pl.multiple_of((2 * block + side) * half, 16), half)

    def send(src, dst, send_sem, recv_sem, peer):
        copy = pltpu.make_async_remote_copy(src, dst, send_sem, recv_sem, device_id={"dp": peer}, device_id_type=MESH)
        copy.start()
        pending.append(copy.wait_send)
        return copy

    def local(src, dst, s):
        copy = pltpu.make_async_copy(src, dst, s)
        copy.start()
        return copy

    sent, loads, steps = {}, {}, {}

    def first(c):
        k, l = chunks[c]
        for side in (0, 1):
            sent["far", c, side] = send(
                g[k].at[0, l, rows(k, opposite, side)], far[k].at[l, side], sem["far_s"].at[c, side], sem["far_r"].at[c, side], ahead[side]
            )
        for side in (0, 1):
            sent["dir", c, side] = send(
                g[k].at[0, l, rows(k, behind[side], side)], direct[k].at[l, side], sem["dir_s"].at[c, side], sem["dir_r"].at[c, side], behind[side]
            )
        for side in (0, 1):
            loads["term", c, side] = local(g[k].at[0, l, rows(k, ahead[side], side)], term[k].at[l, side], sem["term"].at[c, side])
        for side in (0, 1):
            loads["own", c, side] = local(g[k].at[0, l, rows(k, me, side)], own[k].at[l, side], sem["own"].at[c, side])
            loads["w", c, side] = local(w[k].at[l, rows(k, me, side)], new[k].at[l, side], sem["w"].at[c, side])

    def load_moments(c, side):
        k, l = chunks[c]
        half = far[k].shape[2]
        here = pl.ds(side * half, half)
        steps[c, side] = (
            local(m[k].at[l, here], m_buf[k].at[side], sem["m"].at[c, side]),
            local(v[k].at[l, here], v_buf[k].at[side], sem["v"].at[c, side]),
        )

    def relay(c):
        k, l = chunks[c]
        for side in (0, 1):
            sent["far", c, side].wait_recv()
            loads["term", c, side].wait()
            sums, mine = far[k].at[l, side], term[k].at[l, side]

            def add(r, cols):
                sums[r, cols] = (sums[r, cols].astype(F32) + mine[r, cols].astype(F32)).astype(BF16)

            tiled(sums.shape, add)
            sent["rel", c, side] = send(sums, rel[k].at[l, side], sem["rel_s"].at[c, side], sem["rel_r"].at[c, side], ahead[side])

    def step(c):
        k, l = chunks[c]
        half = far[k].shape[2]
        for side in (0, 1):
            sent["dir", c, side].wait_recv()
            sent["rel", c, side].wait_recv()
            loads["own", c, side].wait()
            loads["w", c, side].wait()
            for load in steps[c, side]:
                load.wait()
            a, b, o, x = (array[k].at[l, side] for array in (rel, direct, own, new))
            ms, vs = m_buf[k].at[side], v_buf[k].at[side]

            def update(r, cols):
                total = (a[r, cols].astype(F32) + b[r, cols].astype(F32) + o[r, cols].astype(F32)).astype(BF16)
                o[r, cols] = total
                m_new, v_new = moments(ms[r, cols], vs[r, cols], total.astype(F32))
                x[r, cols] = weight(x[r, cols].astype(F32), m_new, v_new).astype(BF16)

            tiled(o.shape, update)
            here = pl.ds(side * half, half)
            pending.append(local(o, g_out[k].at[l, here], sem["g_out"].at[c, side]).wait)
            if gathered[k]:
                place = w_out[k].at[l, rows(k, me, side)]
                for way, peer in enumerate((ahead[side], behind[side])):
                    sent["near", c, side, way] = send(x, place, sem["near_s"].at[c, side, way], sem["near_r"].at[c, side, way], peer)
                pending.append(local(x, place, sem["w_out"].at[c, side, 0]).wait)
            else:
                for i, (*starts, size) in enumerate(cuts(half)):
                    pending.append(local(x.at[pl.ds(starts[side], size)], w_out[k][i][side].at[l], sem["w_out"].at[c, side, i]).wait)
            if c + 1 < len(chunks):
                load_moments(c + 1, side)

    def forward(c):
        k, l = chunks[c]
        if not gathered[k]:
            return
        for side in (0, 1):
            sent["near", c, side, 0].wait_recv()
            place = w_out[k].at[l, rows(k, behind[side], side)]
            sent["fwd", c, side] = send(place, place, sem["fwd_s"].at[c, side], sem["fwd_r"].at[c, side], ahead[side])

    last = len(chunks)
    for c in range(min(2, last)):
        first(c)
    for side in (0, 1):
        load_moments(0, side)
    for c in range(last + 2):
        if c + 2 < last:
            first(c + 2)
        if c < last:
            relay(c)
        if 0 <= c - 1 < last:
            step(c - 1)
        if 0 <= c - 2 < last:
            forward(c - 2)
    for key, copy in sent.items():
        if key[0] == "fwd" or (key[0] == "near" and key[3] == 1):
            copy.wait_recv()
    for wait in pending:
        wait()


def reduce_and_step(n, gathered, terms, weights, m, v):
    layers = m[0].shape[0]
    count = len(terms)
    chunks = count * layers
    pieces = [(layers, 2, one.shape[1] // 2, one.shape[2]) for one in m]
    blocks = [jax.ShapeDtypeStruct(one.shape, BF16) for one in m]
    new = []
    for w, piece, whole in zip(weights, pieces, gathered, strict=True):
        if whole:
            new.append(jax.ShapeDtypeStruct(w.shape, BF16))
        else:
            new += [jax.ShapeDtypeStruct((layers, size, piece[3]), BF16) for *_, size in cuts(piece[2]) for _ in range(2)]
    out_shape = blocks + new
    sems = [pltpu.SemaphoreType.DMA((chunks, 2, 2) if name in BOTH_WAYS else (chunks, 2)) for name in SEMAPHORES[:-1]]
    sems.append(pltpu.SemaphoreType.REGULAR((2,)))
    return pl.pallas_call(
        functools.partial(kernel, n, layers, gathered),
        out_shape=out_shape,
        in_specs=[pl.BlockSpec(memory_space=pl.ANY)] * (4 * count),
        out_specs=[pl.BlockSpec(memory_space=pl.ANY)] * len(out_shape),
        scratch_shapes=[pltpu.VMEM(p, BF16) for _ in range(6) for p in pieces]
        + [pltpu.VMEM(p[1:], F32) for _ in range(2) for p in pieces]
        + sems,
        compiler_params=pltpu.CompilerParams(collective_id=0, has_side_effects=True, vmem_limit_bytes=66_000_000),
        name="reduce_and_step",
    )(*terms, *weights, *m, *v)


def place_kernel(n, spots, *refs):
    count = len(spots)
    pieces, out, bufs = refs[:count], refs[count], refs[count + 1 : 2 * count + 1]
    in_sem, out_sem = refs[2 * count + 1 :]
    me = lax.axis_index("dp")
    half = out.shape[1] // (2 * n)
    loads = []
    for i, piece in enumerate(pieces):
        copy = pltpu.make_async_copy(piece, bufs[i], in_sem.at[i])
        copy.start()
        loads.append(copy)
    stores = []
    for i, (start, side, offset) in enumerate(spots):
        loads[i].wait()
        row = pl.multiple_of((2 * lax.rem(me + offset, n) + side) * half + start, 16)
        copy = pltpu.make_async_copy(bufs[i], out.at[:, pl.ds(row, bufs[i].shape[1])], out_sem.at[i])
        copy.start()
        stores.append(copy)
    for copy in stores:
        copy.wait()


def place(n, shape, pieces):
    spots = tuple(pieces)
    moved = 4 * sum(piece.size for piece in pieces.values())
    return pl.pallas_call(
        functools.partial(place_kernel, n, spots),
        out_shape=jax.ShapeDtypeStruct(shape, BF16),
        in_specs=[pl.BlockSpec(memory_space=pl.ANY)] * len(spots),
        out_specs=pl.BlockSpec(memory_space=pl.ANY),
        scratch_shapes=[pltpu.VMEM(piece.shape, BF16) for piece in pieces.values()] + [pltpu.SemaphoreType.DMA((len(spots),))] * 2,
        cost_estimate=pl.CostEstimate(flops=moved, bytes_accessed=moved, transcendentals=0),
        name="place",
    )(*pieces.values())


def carry_kernel(parts, *refs):
    count = (len(refs) - 2) // 3
    src, out, buf = (refs[i * count : (i + 1) * count] for i in range(3))
    in_sem, out_sem = refs[3 * count :]
    layers, depth, _ = src[0].shape
    rows = depth // parts
    spots = [(k, l, pl.ds(i * rows, rows)) for k in range(count) for l in range(layers) for i in range(parts)]
    loads = [pltpu.make_async_copy(src[k].at[l, here], buf[k].at[l, here], in_sem.at[i]) for i, (k, l, here) in enumerate(spots)]
    stores = [pltpu.make_async_copy(buf[k].at[l, here], out[k].at[l, here], out_sem.at[i]) for i, (k, l, here) in enumerate(spots)]
    for load in loads:
        load.start()
    for load, store in zip(loads, stores, strict=True):
        load.wait()
        store.start()
    for store in stores:
        store.wait()


def carry(arrays):
    w, count = arrays[0], len(arrays)
    parts = next(k for k in range(8, 0, -1) if w.shape[1] % (16 * k) == 0)
    moved = 4 * w.size * count
    return pl.pallas_call(
        functools.partial(carry_kernel, parts),
        out_shape=[jax.ShapeDtypeStruct(w.shape, w.dtype)] * count,
        in_specs=[pl.BlockSpec(memory_space=pl.ANY)] * count,
        out_specs=[pl.BlockSpec(memory_space=pl.ANY)] * count,
        scratch_shapes=[pltpu.VMEM(w.shape, w.dtype)] * count + [pltpu.SemaphoreType.DMA((count * w.shape[0] * parts,))] * 2,
        cost_estimate=pl.CostEstimate(flops=moved, bytes_accessed=moved, transcendentals=0),
        name="carry",
    )(*arrays)


def gather(n, shape, own):
    half = shape[1] // (2 * n)
    right, left = ([(i, (i + way) % n) for i in range(n)] for way in (1, n - 1))
    near, far = {}, {}
    for i, (*starts, _) in enumerate(cuts(half)):
        for side, ahead in enumerate((right, left)):
            near[starts[side], side, 0] = own[i][side]
            near[starts[side], side, (n - 1, 1)[side]] = lax.ppermute(own[i][side], "dp", ahead)
        for side, behind in enumerate((left, right)):
            near[starts[side], side, (1, n - 1)[side]] = lax.ppermute(own[i][side], "dp", behind)
    for i, (*starts, _) in enumerate(cuts(half)):
        for side, ahead in enumerate((right, left)):
            far[i, side] = lax.ppermute(near[starts[side], side, (n - 1, 1)[side]], "dp", ahead)
    whole = place(n, shape, near)
    opposite = lax.rem(lax.axis_index("dp") + 2, n)
    for i, (*starts, _) in enumerate(cuts(half)):
        row = 2 * opposite * half
        if i == 0:
            for side in (0, 1):
                whole = lax.dynamic_update_slice(whole, far[i, side], (0, row + side * half + starts[side], 0))
        else:
            whole = lax.dynamic_update_slice(whole, jnp.concatenate([far[i, 0], far[i, 1]], 1), (0, row + starts[0], 0))
    return whole


GATHERED = (True, True, False)


def solution(mesh):
    n = mesh.shape["dp"]

    def inner(*arrays):
        terms, weights, m, v = (arrays[i : i + 3] for i in (0, 3, 6, 9))
        out = list(reduce_and_step(n, GATHERED, terms, weights, m, v))
        sums = [out.pop(0) for _ in range(3)]
        held, new, pairs = [], [], []
        for k, whole in enumerate(GATHERED):
            pairs.append(moments(m[k], v[k], sums[k].astype(F32)))
            if whole:
                held.append(out.pop(0))
            else:
                new.append(gather(n, weights[k].shape, [[out.pop(0) for _ in range(2)] for _ in cuts(m[k].shape[1] // 2)]))
        new = [*carry(held), *new]
        return (*new, *(one[0] for one in pairs), *(one[1] for one in pairs))

    all_of, cut = P(None, None, None), P(None, "dp", None)
    return jax.shard_map(
        inner,
        mesh=mesh,
        in_specs=(P(("rep", "dp"), None, None, None),) * 3 + (all_of,) * 3 + (cut,) * 6,
        out_specs=(P("rep", None, None),) * 3 + (P("rep", "dp", None),) * 6,
        check_vma=False,
    )
```

```python
import functools

import jax
import jax.numpy as jnp
from jax import lax
from jax.experimental import pallas as pl
from jax.experimental.pallas import tpu as pltpu
from jax.sharding import PartitionSpec as P


MESH = pl.DeviceIdType.MESH
BF16, F32 = jnp.bfloat16, jnp.float32
SENT = ("far_s", "far_r", "rel_s", "rel_r", "dir_s", "dir_r", "fwd_s", "fwd_r")
LOCAL = ("term", "own", "w", "m", "v", "g_out")
BOTH_WAYS = ("near_s", "near_r", "w_out")
SEMAPHORES = (*SENT, *LOCAL, *BOTH_WAYS, "again")
LATER = 5
POOLS = dict(far_s=3, dir_s=3, rel_s=3, fwd_s=2, near_s=2, term=3, own=4, w=4, m=1, v=1, g_out=2, w_out=2)


def moments(m, v, g):
    return 0.9 * m + 0.1 * g, 0.95 * v + 0.05 * g * g


def weight(w, m, v):
    return w - 0.02 * (m * lax.rsqrt(v + 1e-8) + 0.1 * w)


def columns(width):
    parts = -(-width // 1024)
    while width % (parts * 128):
        parts += 1
    return [slice(i * (width // parts), (i + 1) * (width // parts)) for i in range(parts)]


def cuts(half):
    last = max(16, half // 5 // 16 * 16)
    return (0, last, half - last), (half - last, 0, last)


def tiled(shape, body):
    def row(i, carry):
        rows = pl.ds(pl.multiple_of(i * 16, 16), 16)
        for cols in columns(shape[1]):
            body(rows, cols)
        return carry

    lax.fori_loop(0, shape[0] // 16, row, 0)


def kernel(n, layers, gathered, *refs):
    count = len(gathered)
    refs = list(refs)
    take = lambda k: [refs.pop(0) for _ in range(k)]
    g, w, m, v = take(count), take(count), take(count), take(count)
    g_out = take(count)
    w_out = [take(1)[0] if whole else [take(2) for _ in cuts(w[k].shape[1] // (2 * n))] for k, whole in enumerate(gathered)]
    far, rel, direct, term, own, new = (take(count) for _ in range(6))
    m_buf, v_buf = take(count), take(count)
    sem = dict(zip(SEMAPHORES, refs, strict=True))

    me = lax.axis_index("dp")
    right, left = lax.rem(me + 1, n), lax.rem(me + n - 1, n)
    opposite = lax.rem(me + 2, n)
    ahead, behind = (right, left), (left, right)

    barrier = pltpu.get_barrier_semaphore()
    for peer in (left, right):
        pl.semaphore_signal(barrier, inc=1, device_id={"dp": peer}, device_id_type=MESH)
    pl.semaphore_wait(barrier, 2)
    late = 1 - lax.rem(lax.axis_index("rep"), 2)

    def again(i, carry):
        for peer in (left, right):
            pl.semaphore_signal(sem["again"].at[lax.rem(i, 2)], inc=1, device_id={"dp": peer}, device_id_type=MESH)
        pl.semaphore_wait(sem["again"].at[lax.rem(i, 2)], 2)
        return carry

    lax.fori_loop(0, LATER * late, again, 0)

    chunks = [(k, layer) for k in range(count) for layer in range(layers)]
    busy = {}

    def spot(name, c, *at):
        key = (name, c % sem[name].shape[0], *at)
        if key in busy:
            busy.pop(key)()
        return key, sem[name].at[key[1:]]

    def rows(k, block, side):
        half = far[k].shape[2]
        return pl.ds(pl.multiple_of((2 * block + side) * half, 16), half)

    def send(src, dst, name, c, at, peer):
        key, send_sem = spot(name + "_s", c, *at)
        recv_sem = sem[name + "_r"].at[(c, *at)]
        copy = pltpu.make_async_remote_copy(src, dst, send_sem, recv_sem, device_id={"dp": peer}, device_id_type=MESH)
        copy.start()
        busy[key] = copy.wait_send
        return copy

    def load(src, dst, name, c, side):
        copy = pltpu.make_async_copy(src, dst, spot(name, c, side)[1])
        copy.start()
        return copy

    def store(src, dst, name, c, *at):
        key, done = spot(name, c, *at)
        copy = pltpu.make_async_copy(src, dst, done)
        copy.start()
        busy[key] = copy.wait

    sent, loads, steps = {}, {}, {}

    def first(c):
        k, l = chunks[c]
        for side in (0, 1):
            sent["far", c, side] = send(
                g[k].at[0, l, rows(k, opposite, side)], far[k].at[l, side], "far", c, (side,), ahead[side]
            )
        for side in (0, 1):
            sent["dir", c, side] = send(
                g[k].at[0, l, rows(k, behind[side], side)], direct[k].at[l, side], "dir", c, (side,), behind[side]
            )
        for side in (0, 1):
            loads["term", c, side] = load(g[k].at[0, l, rows(k, ahead[side], side)], term[k].at[l, side], "term", c, side)
        for side in (0, 1):
            loads["own", c, side] = load(g[k].at[0, l, rows(k, me, side)], own[k].at[l, side], "own", c, side)
            loads["w", c, side] = load(w[k].at[l, rows(k, me, side)], new[k].at[l, side], "w", c, side)

    def load_moments(c, side):
        k, l = chunks[c]
        half = far[k].shape[2]
        here = pl.ds(side * half, half)
        steps[c, side] = (
            load(m[k].at[l, here], m_buf[k].at[side], "m", c, side),
            load(v[k].at[l, here], v_buf[k].at[side], "v", c, side),
        )

    def relay(c):
        k, l = chunks[c]
        for side in (0, 1):
            sent["far", c, side].wait_recv()
            loads["term", c, side].wait()
            sums, mine = far[k].at[l, side], term[k].at[l, side]

            def add(r, cols):
                sums[r, cols] = (sums[r, cols].astype(F32) + mine[r, cols].astype(F32)).astype(BF16)

            tiled(sums.shape, add)
            sent["rel", c, side] = send(sums, rel[k].at[l, side], "rel", c, (side,), ahead[side])

    def step(c):
        k, l = chunks[c]
        half = far[k].shape[2]
        for side in (0, 1):
            sent["dir", c, side].wait_recv()
            sent["rel", c, side].wait_recv()
            loads["own", c, side].wait()
            loads["w", c, side].wait()
            for one in steps[c, side]:
                one.wait()
            a, b, o, x = (array[k].at[l, side] for array in (rel, direct, own, new))
            ms, vs = m_buf[k].at[side], v_buf[k].at[side]

            def update(r, cols):
                total = (a[r, cols].astype(F32) + b[r, cols].astype(F32) + o[r, cols].astype(F32)).astype(BF16)
                o[r, cols] = total
                m_new, v_new = moments(ms[r, cols], vs[r, cols], total.astype(F32))
                x[r, cols] = weight(x[r, cols].astype(F32), m_new, v_new).astype(BF16)

            tiled(o.shape, update)
            here = pl.ds(side * half, half)
            store(o, g_out[k].at[l, here], "g_out", c, side)
            if gathered[k]:
                place = w_out[k].at[l, rows(k, me, side)]
                for way, peer in enumerate((ahead[side], behind[side])):
                    sent["near", c, side, way] = send(x, place, "near", c, (side, way), peer)
                store(x, place, "w_out", c, side, 0)
            else:
                for i, (*starts, size) in enumerate(cuts(half)):
                    store(x.at[pl.ds(starts[side], size)], w_out[k][i][side].at[l], "w_out", c, side, i)
            if c + 1 < len(chunks):
                load_moments(c + 1, side)

    def forward(c):
        k, l = chunks[c]
        if not gathered[k]:
            return
        for side in (0, 1):
            sent["near", c, side, 0].wait_recv()
            place = w_out[k].at[l, rows(k, behind[side], side)]
            sent["fwd", c, side] = send(place, place, "fwd", c, (side,), ahead[side])

    last = len(chunks)
    for c in range(min(2, last)):
        first(c)
    for side in (0, 1):
        load_moments(0, side)
    for c in range(last + 2):
        if c + 2 < last:
            first(c + 2)
        if c < last:
            relay(c)
        if 0 <= c - 1 < last:
            step(c - 1)
        if 0 <= c - 2 < last:
            forward(c - 2)
    for key, copy in sent.items():
        if key[0] == "fwd" or (key[0] == "near" and key[3] == 1):
            copy.wait_recv()
    for wait in busy.values():
        wait()


def reduce_and_step(n, gathered, terms, weights, m, v):
    layers = m[0].shape[0]
    count = len(terms)
    chunks = count * layers
    pieces = [(layers, 2, one.shape[1] // 2, one.shape[2]) for one in m]
    blocks = [jax.ShapeDtypeStruct(one.shape, BF16) for one in m]
    new = []
    for w, piece, whole in zip(weights, pieces, gathered, strict=True):
        if whole:
            new.append(jax.ShapeDtypeStruct(w.shape, BF16))
        else:
            new += [jax.ShapeDtypeStruct((layers, size, piece[3]), BF16) for *_, size in cuts(piece[2]) for _ in range(2)]
    out_shape = blocks + new
    whole_chunks = layers * max(k + 1 for k in range(count) if gathered[k])
    depth = {name: POOLS.get(name, whole_chunks if name in ("near_r", "fwd_r") else chunks) for name in SEMAPHORES[:-1]}
    sems = [pltpu.SemaphoreType.DMA((size, 2, 2) if name in BOTH_WAYS else (size, 2)) for name, size in depth.items()]
    sems.append(pltpu.SemaphoreType.REGULAR((2,)))
    return pl.pallas_call(
        functools.partial(kernel, n, layers, gathered),
        out_shape=out_shape,
        in_specs=[pl.BlockSpec(memory_space=pl.ANY)] * (4 * count),
        out_specs=[pl.BlockSpec(memory_space=pl.ANY)] * len(out_shape),
        scratch_shapes=[pltpu.VMEM(p, BF16) for _ in range(6) for p in pieces]
        + [pltpu.VMEM(p[1:], F32) for _ in range(2) for p in pieces]
        + sems,
        compiler_params=pltpu.CompilerParams(collective_id=0, has_side_effects=True, vmem_limit_bytes=66_000_000),
        name="reduce_and_step",
    )(*terms, *weights, *m, *v)


def place_kernel(n, spots, *refs):
    count = len(spots)
    pieces, out, bufs = refs[:count], refs[count], refs[count + 1 : 2 * count + 1]
    in_sem, out_sem = refs[2 * count + 1 :]
    me = lax.axis_index("dp")
    half = out.shape[1] // (2 * n)
    loads = []
    for i, piece in enumerate(pieces):
        copy = pltpu.make_async_copy(piece, bufs[i], in_sem.at[i])
        copy.start()
        loads.append(copy)
    stores = []
    for i, (start, side, offset) in enumerate(spots):
        loads[i].wait()
        row = pl.multiple_of((2 * lax.rem(me + offset, n) + side) * half + start, 16)
        copy = pltpu.make_async_copy(bufs[i], out.at[:, pl.ds(row, bufs[i].shape[1])], out_sem.at[i])
        copy.start()
        stores.append(copy)
    for copy in stores:
        copy.wait()


def place(n, shape, pieces):
    spots = tuple(pieces)
    moved = 4 * sum(piece.size for piece in pieces.values())
    return pl.pallas_call(
        functools.partial(place_kernel, n, spots),
        out_shape=jax.ShapeDtypeStruct(shape, BF16),
        in_specs=[pl.BlockSpec(memory_space=pl.ANY)] * len(spots),
        out_specs=pl.BlockSpec(memory_space=pl.ANY),
        scratch_shapes=[pltpu.VMEM(piece.shape, BF16) for piece in pieces.values()] + [pltpu.SemaphoreType.DMA((len(spots),))] * 2,
        cost_estimate=pl.CostEstimate(flops=moved, bytes_accessed=moved, transcendentals=0),
        name="place",
    )(*pieces.values())


def carry_kernel(parts, *refs):
    count = (len(refs) - 2) // 3
    src, out, buf = (refs[i * count : (i + 1) * count] for i in range(3))
    in_sem, out_sem = refs[3 * count :]
    layers, depth, _ = src[0].shape
    rows = depth // parts
    spots = [(k, l, pl.ds(i * rows, rows)) for k in range(count) for l in range(layers) for i in range(parts)]
    loads = [pltpu.make_async_copy(src[k].at[l, here], buf[k].at[l, here], in_sem.at[i]) for i, (k, l, here) in enumerate(spots)]
    stores = [pltpu.make_async_copy(buf[k].at[l, here], out[k].at[l, here], out_sem.at[i]) for i, (k, l, here) in enumerate(spots)]
    for load in loads:
        load.start()
    for load, store in zip(loads, stores, strict=True):
        load.wait()
        store.start()
    for store in stores:
        store.wait()


def carry(arrays):
    w, count = arrays[0], len(arrays)
    parts = next(k for k in range(8, 0, -1) if w.shape[1] % (16 * k) == 0)
    moved = 4 * w.size * count
    return pl.pallas_call(
        functools.partial(carry_kernel, parts),
        out_shape=[jax.ShapeDtypeStruct(w.shape, w.dtype)] * count,
        in_specs=[pl.BlockSpec(memory_space=pl.ANY)] * count,
        out_specs=[pl.BlockSpec(memory_space=pl.ANY)] * count,
        scratch_shapes=[pltpu.VMEM(w.shape, w.dtype)] * count + [pltpu.SemaphoreType.DMA((count * w.shape[0] * parts,))] * 2,
        cost_estimate=pl.CostEstimate(flops=moved, bytes_accessed=moved, transcendentals=0),
        name="carry",
    )(*arrays)


def gather(n, shape, own):
    half = shape[1] // (2 * n)
    right, left = ([(i, (i + way) % n) for i in range(n)] for way in (1, n - 1))
    near, far = {}, {}
    for i, (*starts, _) in enumerate(cuts(half)):
        for side, ahead in enumerate((right, left)):
            near[starts[side], side, 0] = own[i][side]
            near[starts[side], side, (n - 1, 1)[side]] = lax.ppermute(own[i][side], "dp", ahead)
        for side, behind in enumerate((left, right)):
            near[starts[side], side, (1, n - 1)[side]] = lax.ppermute(own[i][side], "dp", behind)
    for i, (*starts, _) in enumerate(cuts(half)):
        for side, ahead in enumerate((right, left)):
            far[i, side] = lax.ppermute(near[starts[side], side, (n - 1, 1)[side]], "dp", ahead)
    whole = place(n, shape, near)
    opposite = lax.rem(lax.axis_index("dp") + 2, n)
    for i, (*starts, _) in enumerate(cuts(half)):
        row = 2 * opposite * half
        if i == 0:
            for side in (0, 1):
                whole = lax.dynamic_update_slice(whole, far[i, side], (0, row + side * half + starts[side], 0))
        else:
            whole = lax.dynamic_update_slice(whole, jnp.concatenate([far[i, 0], far[i, 1]], 1), (0, row + starts[0], 0))
    return whole


GATHERED = (True, True, False)


def solution(mesh):
    n = mesh.shape["dp"]

    def inner(*arrays):
        terms, weights, m, v = (arrays[i : i + 3] for i in (0, 3, 6, 9))
        out = list(reduce_and_step(n, GATHERED, terms, weights, m, v))
        sums = [out.pop(0) for _ in range(3)]
        held, new, pairs = [], [], []
        for k, whole in enumerate(GATHERED):
            pairs.append(moments(m[k], v[k], sums[k].astype(F32)))
            if whole:
                held.append(out.pop(0))
            else:
                new.append(gather(n, weights[k].shape, [[out.pop(0) for _ in range(2)] for _ in cuts(m[k].shape[1] // 2)]))
        new = [*carry(held), *new]
        return (*new, *(one[0] for one in pairs), *(one[1] for one in pairs))

    all_of, cut = P(None, None, None), P(None, "dp", None)
    return jax.shard_map(
        inner,
        mesh=mesh,
        in_specs=(P(("rep", "dp"), None, None, None),) * 3 + (all_of,) * 3 + (cut,) * 6,
        out_specs=(P("rep", None, None),) * 3 + (P("rep", "dp", None),) * 6,
        check_vma=False,
    )
```

```python
import functools

import jax
import jax.numpy as jnp
from jax import lax
from jax.experimental import pallas as pl
from jax.experimental.pallas import tpu as pltpu
from jax.sharding import PartitionSpec as P


MESH = pl.DeviceIdType.MESH
BF16, F32 = jnp.bfloat16, jnp.float32
SENT = ("far_s", "far_r", "rel_s", "rel_r", "dir_s", "dir_r", "fwd_s", "fwd_r")
LOCAL = ("term", "own", "w", "m", "v", "g_out")
BOTH_WAYS = ("near_s", "near_r", "w_out")
SEMAPHORES = (*SENT, *LOCAL, *BOTH_WAYS, "again")
LATER = 5
POOLS = dict(far_s=3, dir_s=3, rel_s=3, fwd_s=2, near_s=2, term=3, own=4, w=4, m=1, v=1, g_out=2, w_out=2)


def moments(m, v, g):
    return 0.9 * m + 0.1 * g, 0.95 * v + 0.05 * g * g


def weight(w, m, v):
    return w - 0.02 * (m * lax.rsqrt(v + 1e-8) + 0.1 * w)


def columns(width):
    parts = -(-width // 1024)
    while width % (parts * 128):
        parts += 1
    return [slice(i * (width // parts), (i + 1) * (width // parts)) for i in range(parts)]


def cuts(half):
    last = max(16, half // 5 // 16 * 16)
    return (0, last, half - last), (half - last, 0, last)


def tiled(shape, body):
    def row(i, carry):
        rows = pl.ds(pl.multiple_of(i * 16, 16), 16)
        for cols in columns(shape[1]):
            body(rows, cols)
        return carry

    lax.fori_loop(0, shape[0] // 16, row, 0)


def kernel(n, layers, gathered, *refs):
    count = len(gathered)
    refs = list(refs)
    take = lambda k: [refs.pop(0) for _ in range(k)]
    g, w, m, v = take(count), take(count), take(count), take(count)
    g_out = take(count)
    w_out = [take(1)[0] if whole else [take(2) for _ in cuts(w[k].shape[1] // (2 * n))] for k, whole in enumerate(gathered)]
    far, rel, direct, term, own, new = (take(count) for _ in range(6))
    m_buf, v_buf = take(count), take(count)
    sem = dict(zip(SEMAPHORES, refs, strict=True))

    me = lax.axis_index("dp")
    right, left = lax.rem(me + 1, n), lax.rem(me + n - 1, n)
    opposite = lax.rem(me + 2, n)
    ahead, behind = (right, left), (left, right)

    barrier = pltpu.get_barrier_semaphore()
    for peer in (left, right):
        pl.semaphore_signal(barrier, inc=1, device_id={"dp": peer}, device_id_type=MESH)
    pl.semaphore_wait(barrier, 2)
    late = 1 - lax.rem(lax.axis_index("rep"), 2)

    def again(i, carry):
        for peer in (left, right):
            pl.semaphore_signal(sem["again"].at[lax.rem(i, 2)], inc=1, device_id={"dp": peer}, device_id_type=MESH)
        pl.semaphore_wait(sem["again"].at[lax.rem(i, 2)], 2)
        return carry

    lax.fori_loop(0, LATER * late, again, 0)

    chunks = [(k, layer) for k in range(count) for layer in range(layers)]
    busy = {}

    def spot(name, c, *at):
        key = (name, c % sem[name].shape[0], *at)
        if key in busy:
            busy.pop(key)()
        return key, sem[name].at[key[1:]]

    def rows(k, block, side):
        half = far[k].shape[2]
        return pl.ds(pl.multiple_of((2 * block + side) * half, 16), half)

    def send(src, dst, name, c, at, peer):
        key, send_sem = spot(name + "_s", c, *at)
        recv_sem = sem[name + "_r"].at[(c, *at)]
        copy = pltpu.make_async_remote_copy(src, dst, send_sem, recv_sem, device_id={"dp": peer}, device_id_type=MESH)
        copy.start()
        busy[key] = copy.wait_send
        return copy

    def load(src, dst, name, c, side):
        copy = pltpu.make_async_copy(src, dst, spot(name, c, side)[1])
        copy.start()
        return copy

    def store(src, dst, name, c, *at):
        key, done = spot(name, c, *at)
        copy = pltpu.make_async_copy(src, dst, done)
        copy.start()
        busy[key] = copy.wait

    sent, loads, steps = {}, {}, {}

    def first(c):
        k, l = chunks[c]
        for side in (1, 0):
            sent["far", c, side] = send(
                g[k].at[0, l, rows(k, opposite, side)], far[k].at[l, side], "far", c, (side,), ahead[side]
            )
        for side in (1, 0):
            sent["dir", c, side] = send(
                g[k].at[0, l, rows(k, behind[side], side)], direct[k].at[l, side], "dir", c, (side,), behind[side]
            )
        for side in (1, 0):
            loads["term", c, side] = load(g[k].at[0, l, rows(k, ahead[side], side)], term[k].at[l, side], "term", c, side)
        for side in (1, 0):
            loads["own", c, side] = load(g[k].at[0, l, rows(k, me, side)], own[k].at[l, side], "own", c, side)
            loads["w", c, side] = load(w[k].at[l, rows(k, me, side)], new[k].at[l, side], "w", c, side)

    def load_moments(c, side):
        k, l = chunks[c]
        half = far[k].shape[2]
        here = pl.ds(side * half, half)
        steps[c, side] = (
            load(m[k].at[l, here], m_buf[k].at[side], "m", c, side),
            load(v[k].at[l, here], v_buf[k].at[side], "v", c, side),
        )

    def relay(c):
        k, l = chunks[c]
        for side in (1, 0):
            sent["far", c, side].wait_recv()
            loads["term", c, side].wait()
            sums, mine = far[k].at[l, side], term[k].at[l, side]

            def add(r, cols):
                sums[r, cols] = (sums[r, cols].astype(F32) + mine[r, cols].astype(F32)).astype(BF16)

            tiled(sums.shape, add)
            sent["rel", c, side] = send(sums, rel[k].at[l, side], "rel", c, (side,), ahead[side])

    def step(c):
        k, l = chunks[c]
        half = far[k].shape[2]
        for side in (1, 0):
            sent["dir", c, side].wait_recv()
            sent["rel", c, side].wait_recv()
            loads["own", c, side].wait()
            loads["w", c, side].wait()
            for one in steps[c, side]:
                one.wait()
            a, b, o, x = (array[k].at[l, side] for array in (rel, direct, own, new))
            ms, vs = m_buf[k].at[side], v_buf[k].at[side]

            def update(r, cols):
                total = (a[r, cols].astype(F32) + b[r, cols].astype(F32) + o[r, cols].astype(F32)).astype(BF16)
                o[r, cols] = total
                m_new, v_new = moments(ms[r, cols], vs[r, cols], total.astype(F32))
                x[r, cols] = weight(x[r, cols].astype(F32), m_new, v_new).astype(BF16)

            tiled(o.shape, update)
            here = pl.ds(side * half, half)
            store(o, g_out[k].at[l, here], "g_out", c, side)
            if gathered[k]:
                place = w_out[k].at[l, rows(k, me, side)]
                for way, peer in enumerate((ahead[side], behind[side])):
                    sent["near", c, side, way] = send(x, place, "near", c, (side, way), peer)
                store(x, place, "w_out", c, side, 0)
            else:
                for i, (*starts, size) in enumerate(cuts(half)):
                    store(x.at[pl.ds(starts[side], size)], w_out[k][i][side].at[l], "w_out", c, side, i)
            if c + 1 < len(chunks):
                load_moments(c + 1, side)

    def forward(c):
        k, l = chunks[c]
        if not gathered[k]:
            return
        for side in (0, 1):
            sent["near", c, side, 0].wait_recv()
            place = w_out[k].at[l, rows(k, behind[side], side)]
            sent["fwd", c, side] = send(place, place, "fwd", c, (side,), ahead[side])

    last = len(chunks)
    for c in range(min(2, last)):
        first(c)
    for side in (0, 1):
        load_moments(0, side)
    for c in range(last + 2):
        if c + 2 < last:
            first(c + 2)
        if c < last:
            relay(c)
        if 0 <= c - 1 < last:
            step(c - 1)
        if 0 <= c - 2 < last:
            forward(c - 2)
    for key, copy in sent.items():
        if key[0] == "fwd" or (key[0] == "near" and key[3] == 1):
            copy.wait_recv()
    for wait in busy.values():
        wait()


def reduce_and_step(n, gathered, terms, weights, m, v):
    layers = m[0].shape[0]
    count = len(terms)
    chunks = count * layers
    pieces = [(layers, 2, one.shape[1] // 2, one.shape[2]) for one in m]
    blocks = [jax.ShapeDtypeStruct(one.shape, BF16) for one in m]
    new = []
    for w, piece, whole in zip(weights, pieces, gathered, strict=True):
        if whole:
            new.append(jax.ShapeDtypeStruct(w.shape, BF16))
        else:
            new += [jax.ShapeDtypeStruct((layers, size, piece[3]), BF16) for *_, size in cuts(piece[2]) for _ in range(2)]
    out_shape = blocks + new
    whole_chunks = layers * max(k + 1 for k in range(count) if gathered[k])
    depth = {name: POOLS.get(name, whole_chunks if name in ("near_r", "fwd_r") else chunks) for name in SEMAPHORES[:-1]}
    sems = [pltpu.SemaphoreType.DMA((size, 2, 2) if name in BOTH_WAYS else (size, 2)) for name, size in depth.items()]
    sems.append(pltpu.SemaphoreType.REGULAR((2,)))
    return pl.pallas_call(
        functools.partial(kernel, n, layers, gathered),
        out_shape=out_shape,
        in_specs=[pl.BlockSpec(memory_space=pl.ANY)] * (4 * count),
        out_specs=[pl.BlockSpec(memory_space=pl.ANY)] * len(out_shape),
        scratch_shapes=[pltpu.VMEM(p, BF16) for _ in range(6) for p in pieces]
        + [pltpu.VMEM(p[1:], F32) for _ in range(2) for p in pieces]
        + sems,
        compiler_params=pltpu.CompilerParams(collective_id=0, has_side_effects=True, vmem_limit_bytes=66_000_000),
        name="reduce_and_step",
    )(*terms, *weights, *m, *v)


def place_kernel(n, spots, *refs):
    count = len(spots)
    pieces, out, bufs = refs[:count], refs[count], refs[count + 1 : 2 * count + 1]
    in_sem, out_sem = refs[2 * count + 1 :]
    me = lax.axis_index("dp")
    half = out.shape[1] // (2 * n)
    loads = []
    for i, piece in enumerate(pieces):
        copy = pltpu.make_async_copy(piece, bufs[i], in_sem.at[i])
        copy.start()
        loads.append(copy)
    stores = []
    for i, (start, side, offset) in enumerate(spots):
        loads[i].wait()
        row = pl.multiple_of((2 * lax.rem(me + offset, n) + side) * half + start, 16)
        copy = pltpu.make_async_copy(bufs[i], out.at[:, pl.ds(row, bufs[i].shape[1])], out_sem.at[i])
        copy.start()
        stores.append(copy)
    for copy in stores:
        copy.wait()


def place(n, shape, pieces):
    spots = tuple(pieces)
    moved = 4 * sum(piece.size for piece in pieces.values())
    return pl.pallas_call(
        functools.partial(place_kernel, n, spots),
        out_shape=jax.ShapeDtypeStruct(shape, BF16),
        in_specs=[pl.BlockSpec(memory_space=pl.ANY)] * len(spots),
        out_specs=pl.BlockSpec(memory_space=pl.ANY),
        scratch_shapes=[pltpu.VMEM(piece.shape, BF16) for piece in pieces.values()] + [pltpu.SemaphoreType.DMA((len(spots),))] * 2,
        cost_estimate=pl.CostEstimate(flops=moved, bytes_accessed=moved, transcendentals=0),
        name="place",
    )(*pieces.values())


def carry_kernel(parts, *refs):
    count = (len(refs) - 2) // 3
    src, out, buf = (refs[i * count : (i + 1) * count] for i in range(3))
    in_sem, out_sem = refs[3 * count :]
    layers, depth, _ = src[0].shape
    rows = depth // parts
    spots = [(k, l, pl.ds(i * rows, rows)) for k in range(count) for l in range(layers) for i in range(parts)]
    loads = [pltpu.make_async_copy(src[k].at[l, here], buf[k].at[l, here], in_sem.at[i]) for i, (k, l, here) in enumerate(spots)]
    stores = [pltpu.make_async_copy(buf[k].at[l, here], out[k].at[l, here], out_sem.at[i]) for i, (k, l, here) in enumerate(spots)]
    for load in loads:
        load.start()
    for load, store in zip(loads, stores, strict=True):
        load.wait()
        store.start()
    for store in stores:
        store.wait()


def carry(arrays):
    w, count = arrays[0], len(arrays)
    parts = next(k for k in range(8, 0, -1) if w.shape[1] % (16 * k) == 0)
    moved = 4 * w.size * count
    return pl.pallas_call(
        functools.partial(carry_kernel, parts),
        out_shape=[jax.ShapeDtypeStruct(w.shape, w.dtype)] * count,
        in_specs=[pl.BlockSpec(memory_space=pl.ANY)] * count,
        out_specs=[pl.BlockSpec(memory_space=pl.ANY)] * count,
        scratch_shapes=[pltpu.VMEM(w.shape, w.dtype)] * count + [pltpu.SemaphoreType.DMA((count * w.shape[0] * parts,))] * 2,
        cost_estimate=pl.CostEstimate(flops=moved, bytes_accessed=moved, transcendentals=0),
        name="carry",
    )(*arrays)


def gather(n, shape, own):
    half = shape[1] // (2 * n)
    right, left = ([(i, (i + way) % n) for i in range(n)] for way in (1, n - 1))
    near, far = {}, {}
    for i, (*starts, _) in enumerate(cuts(half)):
        for side, ahead in enumerate((right, left)):
            near[starts[side], side, 0] = own[i][side]
            near[starts[side], side, (n - 1, 1)[side]] = lax.ppermute(own[i][side], "dp", ahead)
        for side, behind in enumerate((left, right)):
            near[starts[side], side, (1, n - 1)[side]] = lax.ppermute(own[i][side], "dp", behind)
    for i, (*starts, _) in enumerate(cuts(half)):
        for side, ahead in enumerate((right, left)):
            far[i, side] = lax.ppermute(near[starts[side], side, (n - 1, 1)[side]], "dp", ahead)
    whole = place(n, shape, near)
    opposite = lax.rem(lax.axis_index("dp") + 2, n)
    for i, (*starts, _) in enumerate(cuts(half)):
        row = 2 * opposite * half
        if i == 0:
            for side in (0, 1):
                whole = lax.dynamic_update_slice(whole, far[i, side], (0, row + side * half + starts[side], 0))
        else:
            whole = lax.dynamic_update_slice(whole, jnp.concatenate([far[i, 0], far[i, 1]], 1), (0, row + starts[0], 0))
    return whole


GATHERED = (True, True, False)


def solution(mesh):
    n = mesh.shape["dp"]

    def inner(*arrays):
        terms, weights, m, v = (arrays[i : i + 3] for i in (0, 3, 6, 9))
        out = list(reduce_and_step(n, GATHERED, terms, weights, m, v))
        sums = [out.pop(0) for _ in range(3)]
        held, new, pairs = [], [], []
        for k, whole in enumerate(GATHERED):
            pairs.append(moments(m[k], v[k], sums[k].astype(F32)))
            if whole:
                held.append(out.pop(0))
            else:
                new.append(gather(n, weights[k].shape, [[out.pop(0) for _ in range(2)] for _ in cuts(m[k].shape[1] // 2)]))
        new = [*carry(held), *new]
        return (*new, *(one[0] for one in pairs), *(one[1] for one in pairs))

    all_of, cut = P(None, None, None), P(None, "dp", None)
    return jax.shard_map(
        inner,
        mesh=mesh,
        in_specs=(P(("rep", "dp"), None, None, None),) * 3 + (all_of,) * 3 + (cut,) * 6,
        out_specs=(P("rep", None, None),) * 3 + (P("rep", "dp", None),) * 6,
        check_vma=False,
    )
```
